16 devices in a mesh: fsdp: 16 (over z, y, x, core).
Axes of the slice: x: 2, y: 2, z: 2, core: 2. Of those that a mesh axis runs over, the one named last changes fastest.
Arguments:
- x_saved: bfloat16 [2, 2, 16, 2048, 512], P(None, None, 'fsdp')
- grad_out: bfloat16 [2, 16, 2048, 512], P(None, 'fsdp')
- x_next: bfloat16 [2, 16, 2048, 512], P(None, 'fsdp')
- w_up: bfloat16 [2, 2, 512, 2048], replicated
- w_down: bfloat16 [2, 2, 2048, 512], replicated
- acc_up: float32 [2, 2, 512, 2048], P(None, None, 'fsdp')
- acc_down: float32 [2, 2, 2048, 512], P(None, None, 'fsdp')
- master_up: float32 [2, 2, 512, 2048], P(None, None, 'fsdp')
- master_down: float32 [2, 2, 2048, 512], P(None, None, 'fsdp')
- moment1_up: float32 [2, 2, 512, 2048], P(None, None, 'fsdp')
- moment1_down: float32 [2, 2, 2048, 512], P(None, None, 'fsdp')
- moment2_up: float32 [2, 2, 512, 2048], P(None, None, 'fsdp')
- moment2_down: float32 [2, 2, 2048, 512], P(None, None, 'fsdp')
Outputs:
- output 1: float32 [2, 2, 512, 2048], P(None, None, 'fsdp')
- output 2: float32 [2, 2, 2048, 512], P(None, None, 'fsdp')
- output 3: float32 [2, 2, 512, 2048], P(None, None, 'fsdp')
- output 4: float32 [2, 2, 2048, 512], P(None, None, 'fsdp')
- output 5: float32 [2, 2, 512, 2048], P(None, None, 'fsdp')
- output 6: float32 [2, 2, 2048, 512], P(None, None, 'fsdp')
- output 7: bfloat16 [2, 16, 2048, 512], P(None, 'fsdp')
All inputs are finite; a program needn't handle non-finite values.
Results may differ from the reference program's by a relative error of at most 0.00799662.
Values are sent between devices in bfloat16 or wider.
A program may use at most 1 GiB of HBM per device.

```python
import functools
import jax
import jax.numpy as jnp
from jax import lax

D = 512
FF = 2048
BATCH = 16
SEQ_LEN = 2048
GROUPS = 16
STAGES = 2
LAYERS = 2
MICROBATCHES = 2
ADAM_STEP = 2
TOKENS = BATCH // GROUPS * SEQ_LEN
LEARN_RATE = 0.005
BETA_ONE = 0.9
BETA_TWO = 0.95
ADAM_EPS = 1e-8
WEIGHT_DECAY = 0.1


def setup_inputs(seed: int = 0) -> dict:
    key_list = jax.random.split(jax.random.key(seed), 13)
    row_count = BATCH * SEQ_LEN
    scale_up = 0.3 * row_count ** 0.5
    scale_down = 0.7 * row_count ** 0.5
    tok_shape = (STAGES, BATCH, SEQ_LEN, D)
    up_shape = (STAGES, LAYERS, D, FF)
    down_shape = (STAGES, LAYERS, FF, D)
    x_saved = jax.random.normal(key_list[0], (STAGES, LAYERS, BATCH, SEQ_LEN, D), jnp.float32).astype(jnp.bfloat16)
    grad_out = jax.random.normal(key_list[1], tok_shape, jnp.float32).astype(jnp.bfloat16)
    x_next = jax.random.normal(key_list[2], tok_shape, jnp.float32).astype(jnp.bfloat16)
    w_up = (jax.random.normal(key_list[3], up_shape, jnp.float32) * D ** -0.5).astype(jnp.bfloat16)
    w_down = (jax.random.normal(key_list[4], down_shape, jnp.float32) * FF ** -0.5).astype(jnp.bfloat16)
    acc_up = jax.random.normal(key_list[5], up_shape, jnp.float32) * scale_up
    acc_down = jax.random.normal(key_list[6], down_shape, jnp.float32) * scale_down
    master_up = jax.random.normal(key_list[7], up_shape, jnp.float32) * D ** -0.5
    master_down = jax.random.normal(key_list[8], down_shape, jnp.float32) * FF ** -0.5
    moment1_up = jax.random.normal(key_list[9], up_shape, jnp.float32) * (0.05 * scale_up)
    moment1_down = jax.random.normal(key_list[10], down_shape, jnp.float32) * (0.05 * scale_down)
    moment2_up = jax.random.uniform(key_list[11], up_shape, jnp.float32, 0.02, 0.06) * scale_up ** 2
    moment2_down = jax.random.uniform(key_list[12], down_shape, jnp.float32, 0.02, 0.06) * scale_down ** 2
    return {'x_saved': x_saved, 'grad_out': grad_out, 'x_next': x_next, 'w_up': w_up, 'w_down': w_down, 'acc_up': acc_up, 'acc_down': acc_down, 'master_up': master_up, 'master_down': master_down, 'moment1_up': moment1_up, 'moment1_down': moment1_down, 'moment2_up': moment2_up, 'moment2_down': moment2_down}


def backward_layer(x_in, cotangent, w_one, w_two):
    hidden = jnp.dot(x_in, w_one, preferred_element_type=jnp.float32)
    gelu_out, gelu_vjp = jax.vjp(jax.nn.gelu, hidden)
    gelu_out = gelu_out.astype(jnp.bfloat16)
    grad_act = jnp.dot(cotangent, w_two.T, preferred_element_type=jnp.float32)
    grad_hidden = gelu_vjp(grad_act)[0].astype(jnp.bfloat16)
    part_down = jnp.dot(gelu_out.T, cotangent, preferred_element_type=jnp.float32)
    part_up = jnp.dot(x_in.T, grad_hidden, preferred_element_type=jnp.float32)
    return part_up, part_down, grad_hidden


def stage_grads(x_layers, grad_top, up_stack, down_stack):
    x_blocks = jnp.swapaxes(x_layers.reshape(LAYERS, GROUPS, TOKENS, D), 0, 1)
    grad_blocks = grad_top.reshape(GROUPS, TOKENS, D)

    def scan_body(carry, block_pair):
        sum_up, sum_down = carry
        x_block, cotangent = block_pair
        up_parts = [None] * LAYERS
        down_parts = [None] * LAYERS
        for layer_id in reversed(range(LAYERS)):
            part_up, part_down, grad_hidden = backward_layer(x_block[layer_id], cotangent, up_stack[layer_id], down_stack[layer_id])
            up_parts[layer_id] = part_up
            down_parts[layer_id] = part_down
            if layer_id > 0:
                cotangent = (cotangent.astype(jnp.float32) + jnp.dot(grad_hidden, up_stack[layer_id].T, preferred_element_type=jnp.float32)).astype(jnp.bfloat16)
        return (sum_up + jnp.stack(up_parts), sum_down + jnp.stack(down_parts)), None

    start_sums = (jnp.zeros((LAYERS, D, FF), jnp.float32), jnp.zeros((LAYERS, FF, D), jnp.float32))
    final_sums, scan_rest = lax.scan(scan_body, start_sums, (x_blocks, grad_blocks))
    return final_sums


def adam_update(acc_part, grad_new, master, moment_one, moment_two):
    grad_mean = (acc_part + grad_new) / MICROBATCHES
    moment_one = BETA_ONE * moment_one + (1.0 - BETA_ONE) * grad_mean
    moment_two = BETA_TWO * moment_two + (1.0 - BETA_TWO) * grad_mean * grad_mean
    corr_one = 1.0 - BETA_ONE ** ADAM_STEP
    corr_two = 1.0 - BETA_TWO ** ADAM_STEP
    step_dir = (moment_one / corr_one) / (jnp.sqrt(moment_two / corr_two) + ADAM_EPS)
    master = master - LEARN_RATE * (step_dir + WEIGHT_DECAY * master)
    return master, moment_one, moment_two


def forward_rows(x_rows, up_stack, down_stack):
    for layer_id in range(LAYERS):
        hidden = jnp.dot(x_rows, up_stack[layer_id], preferred_element_type=jnp.float32)
        gelu_out = jax.nn.gelu(hidden).astype(jnp.bfloat16)
        mlp_val = jnp.dot(gelu_out, down_stack[layer_id], preferred_element_type=jnp.float32)
        x_rows = (x_rows.astype(jnp.float32) + mlp_val).astype(jnp.bfloat16)
    return x_rows


def reference(x_saved, grad_out, x_next, w_up, w_down, acc_up, acc_down, master_up, master_down, moment1_up, moment1_down, moment2_up, moment2_down):
    grads_up = []
    grads_down = []
    for stage_id in range(STAGES):
        sum_up, sum_down = stage_grads(x_saved[stage_id], grad_out[stage_id], w_up[stage_id], w_down[stage_id])
        grads_up.append(sum_up)
        grads_down.append(sum_down)
    new_master_up, new_moment1_up, new_moment2_up = adam_update(acc_up, jnp.stack(grads_up), master_up, moment1_up, moment2_up)
    new_master_down, new_moment1_down, new_moment2_down = adam_update(acc_down, jnp.stack(grads_down), master_down, moment1_down, moment2_down)
    new_up = new_master_up.astype(jnp.bfloat16)
    new_down = new_master_down.astype(jnp.bfloat16)
    outs_next = []
    for stage_id in range(STAGES):
        row_blocks = x_next[stage_id].reshape(GROUPS, TOKENS, D)
        moved = lax.map(functools.partial(forward_rows, up_stack=new_up[stage_id], down_stack=new_down[stage_id]), row_blocks)
        outs_next.append(moved.reshape(BATCH, SEQ_LEN, D))
    y_next = jnp.stack(outs_next)
    return (new_master_up, new_master_down, new_moment1_up, new_moment1_down, new_moment2_up, new_moment2_down, y_next)
```

```python
import jax
import jax.numpy as jnp
from jax import lax
from jax.experimental import pallas as pl
from jax.experimental.pallas import tpu as pltpu
from jax.sharding import PartitionSpec as P

LEARN_RATE = 0.005
BETA_ONE = 0.9
BETA_TWO = 0.95
ADAM_EPS = 1e-8
WEIGHT_DECAY = 0.1
MICROBATCHES = 2
ADAM_STEP = 2
CORR_ONE = 1.0 - BETA_ONE ** ADAM_STEP
CORR_TWO = 1.0 - BETA_TWO ** ADAM_STEP

GELU_A = 0.7978845608028654
GELU_B = 0.044715 * GELU_A

MESH = pl.DeviceIdType.MESH
BF16 = jnp.bfloat16
F32 = jnp.float32

NDEV = 16
SEQ = 2048
D = 512
FF = 2048
FC = 256
NCHUNK = FF // FC
UP_ROWS = D // NDEV
DOWN_ROWS = FF // NDEV
TB = 512


def dot_nn(a, b):
    return lax.dot_general(a, b, (((1,), (0,)), ((), ())), preferred_element_type=F32)


def dot_nt(a, b):
    return lax.dot_general(a, b, (((1,), (1,)), ((), ())), preferred_element_type=F32)


def dot_tn(a, b):
    return lax.dot_general(a, b, (((0,), (0,)), ((), ())), preferred_element_type=F32)


def gelu_half(h):
    u = h * h
    return u, 0.5 * jnp.tanh(h * (GELU_B * u + GELU_A)) + 0.5


def gelu_and_grad(h, grad_act):
    u, s = gelu_half(h)
    g = h * s
    slope = s + (g - g * s) * ((6.0 * GELU_B) * u + 2.0 * GELU_A)
    return g.astype(BF16), (grad_act * slope).astype(BF16)


def adam_math(grad_sum, acc, master, mom, vel):
    grad_mean = (acc + grad_sum) / MICROBATCHES
    mom = BETA_ONE * mom + (1.0 - BETA_ONE) * grad_mean
    vel = BETA_TWO * vel + (1.0 - BETA_TWO) * grad_mean * grad_mean
    step_dir = (mom / CORR_ONE) / (jnp.sqrt(vel / CORR_TWO) + ADAM_EPS)
    master = master - LEARN_RATE * (step_dir + WEIGHT_DECAY * master)
    return master, mom, vel


def step_kernel(x_saved, grad_out, x_next, w_up, w_down, acc_up, acc_dn, mas_up, mas_dn, mo_up, mo_dn, ve_up, ve_dn,
                o_mas_up, o_mas_dn, o_mo_up, o_mo_dn, o_ve_up, o_ve_dn, y_out,
                xs_top, xs_low, dyb, dxa, w1, w2, sent_up, sent_dn, recv_up, recv_dn,
                s_acc_up, s_mas_up, s_mo_up, s_ve_up,
                own_up, own_dn, acc1, acc2,
                load_sem, tok_send, tok_recv, rs_send, rs_recv, ag_send, ag_recv, out_sem, y_sem, free_sem):
    me = lax.axis_index('fsdp')
    stage = lax.rem(me, 2)
    other = 1 - stage
    chip = me // 2
    partner = me + 1 - 2 * stage

    def load(i, src, dst):
        return pltpu.make_async_copy(src, dst, load_sem.at[i])

    loads = [
        load(0, w_up.at[stage, 1], w1.at[1]),
        load(1, x_saved.at[stage, 1, 0], xs_top.at[0]),
        load(2, w_down.at[stage, 1], w2.at[1]),
        load(3, grad_out.at[stage, 0], dyb.at[0]),
        load(4, w_up.at[stage, 0], w1.at[0]),
        load(5, x_saved.at[stage, 0, 0], xs_low.at[0]),
        load(6, w_down.at[stage, 0], w2.at[0]),
        load(7, acc_up, s_acc_up), load(8, mas_up, s_mas_up), load(9, mo_up, s_mo_up), load(10, ve_up, s_ve_up),
    ]

    def dn_rows(layer, arr, st):
        return ((layer * 4 + arr) * 2 + st) * DOWN_ROWS

    def dn_view(layer, arr, st):
        return dxa.at[0, pl.ds(dn_rows(layer, arr, st), DOWN_ROWS), :]

    dn_loads = [load(11 + arr * 4 + layer * 2 + st, src.at[st, layer], dn_view(layer, arr, st))
                for arr, src in enumerate((acc_dn, mas_dn, mo_dn, ve_dn)) for layer in range(2) for st in range(2)]
    for c in loads[:4]:
        c.start()

    barrier = pltpu.get_barrier_semaphore()

    def greet(t, _):
        pl.semaphore_signal(barrier, inc=1, device_id=(lax.rem(me + t, NDEV),), device_id_type=MESH)
        return 0

    lax.fori_loop(1, NDEV, greet, 0)
    pl.semaphore_wait(barrier, NDEV - 1)

    def push(i, src, dst):
        return pltpu.make_async_remote_copy(src_ref=src, dst_ref=dst, send_sem=tok_send.at[i], recv_sem=tok_recv.at[i],
                                            device_id=(partner,), device_id_type=MESH)

    pushes = [
        push(0, x_saved.at[other, 1, 0], xs_top.at[1]),
        push(1, grad_out.at[other, 0], dyb.at[1]),
        push(2, x_saved.at[other, 0, 0], xs_low.at[1]),
        push(3, x_next.at[other, 0], xs_top.at[1]),
    ]
    for c in pushes[:3]:
        c.start()
    for c in loads[4:]:
        c.start()
    for c in loads[:4]:
        c.wait()

    def send_up(layer, chunk, dest):
        return pltpu.make_async_remote_copy(
            src_ref=sent_up.at[layer, chunk, pl.ds(pl.multiple_of(dest * UP_ROWS, UP_ROWS), UP_ROWS), :],
            dst_ref=recv_up.at[layer, me, chunk],
            send_sem=rs_send.at[layer, 0], recv_sem=rs_recv.at[layer, 0],
            device_id=(dest,), device_id_type=MESH)

    def send_dn(layer, chunk, core):
        dest = 2 * chunk + core
        return pltpu.make_async_remote_copy(
            src_ref=sent_dn.at[layer, dest],
            dst_ref=recv_dn.at[layer, me],
            send_sem=rs_send.at[layer, 1], recv_sem=rs_recv.at[layer, 1],
            device_id=(dest,), device_id_type=MESH)

    def backward(layer, xs, with_dx, first_waits):
        def chunk_body(t, _):
            chunk = lax.rem(chip + 1 + t, NCHUNK)
            cols = pl.ds(pl.multiple_of(chunk * FC, FC), FC)

            def token_body(q, _):
                @pl.when(jnp.logical_and(t == 0, q == 1))
                def _():
                    for c in first_waits:
                        c.wait_recv()

                @pl.when(q == 0)
                def _():
                    acc1[...] = jnp.zeros_like(acc1)
                    acc2[...] = jnp.zeros_like(acc2)

                x = xs[q]
                dy = dyb[q]
                hidden = dot_nn(x, w1[layer, :, cols])
                grad_act = dot_nt(dy, w2[layer, cols, :])
                act, grad_hidden = gelu_and_grad(hidden, grad_act)
                acc2[...] += dot_tn(act, dy)
                acc1[...] += dot_tn(x, grad_hidden)
                if with_dx:
                    part = dot_nt(grad_hidden, w1[layer, :, cols])

                    @pl.when(t == 0)
                    def _():
                        dxa[q] = part

                    @pl.when(t > 0)
                    def _():
                        dxa[q] += part
                return 0

            lax.fori_loop(0, 2, token_body, 0)
            sent_up[layer, chunk] = acc1[...].astype(BF16)
            for core in range(2):
                sent_dn[layer, 2 * chunk + core] = acc2[core * DOWN_ROWS:(core + 1) * DOWN_ROWS, :].astype(BF16)

            @pl.when(t < NCHUNK - 1)
            def _():
                send_dn(layer, chunk, 0).start()
                send_dn(layer, chunk, 1).start()

            @pl.when(t == NCHUNK - 1)
            def _():
                send_dn(layer, chunk, other).start()
                recv_dn[layer, me] = sent_dn[layer, me]

            def send_body(i, _):
                send_up(layer, chunk, lax.rem(me + i, NDEV)).start()
                return 0

            lax.fori_loop(1, NDEV, send_body, 0)
            recv_up[layer, me, chunk] = sent_up[layer, chunk, pl.ds(pl.multiple_of(me * UP_ROWS, UP_ROWS), UP_ROWS), :]
            return 0

        lax.fori_loop(0, NCHUNK, chunk_body, 0)

    backward(1, xs_top, True, pushes[:2])
    pl.semaphore_signal(free_sem, inc=1, device_id=(partner,), device_id_type=MESH)

    def cot_body(b, _):
        q = b // 4
        rows = pl.ds(pl.multiple_of(lax.rem(b, 4) * TB, TB), TB)
        dyb[q, rows, :] = (dyb[q, rows, :].astype(F32) + dxa[q, rows, :]).astype(BF16)
        return 0

    lax.fori_loop(0, 8, cot_body, 0)
    for c in dn_loads:
        c.start()
    for c in loads[4:7]:
        c.wait()
    backward(0, xs_low, False, pushes[2:3])

    own_next = load(1, x_next.at[stage, 0], xs_top.at[0])
    own_next.start()
    pl.semaphore_wait(free_sem, 1)
    pushes[0].wait_send()
    pushes[3].start()
    for c in loads[7:] + dn_loads:
        c.wait()

    def rs_wait(layer, mat):
        ref = (recv_up if mat == 0 else recv_dn).at[layer, pl.ds(0, NDEV - 1)]
        pltpu.make_async_copy(ref, ref, rs_recv.at[layer, mat]).wait()

    def adam_up(layer):
        def body(chunk, _):
            cols = pl.ds(pl.multiple_of(chunk * FC, FC), FC)
            for st in range(2):
                total = recv_up[layer, st, chunk].astype(F32)
                for k in range(1, 8):
                    total = total + recv_up[layer, 2 * k + st, chunk].astype(F32)
                new = adam_math(total, s_acc_up[st, layer, :, cols], s_mas_up[st, layer, :, cols],
                                s_mo_up[st, layer, :, cols], s_ve_up[st, layer, :, cols])
                s_mas_up[st, layer, :, cols] = new[0]
                s_mo_up[st, layer, :, cols] = new[1]
                s_ve_up[st, layer, :, cols] = new[2]
                own_up[layer, st, :, cols] = new[0].astype(BF16)
            return 0

        lax.fori_loop(0, NCHUNK, body, 0)

    def adam_dn(layer):
        def body(r, _):
            rows = pl.ds(pl.multiple_of(r * 16, 16), 16)
            for st in range(2):
                total = recv_dn[layer, st, rows, :].astype(F32)
                for k in range(1, 8):
                    total = total + recv_dn[layer, 2 * k + st, rows, :].astype(F32)
                at = [pl.ds(pl.multiple_of(dn_rows(layer, arr, st) + r * 16, 16), 16) for arr in range(4)]
                new = adam_math(total, *(dxa[0, a, :] for a in at))
                for a, val in zip(at[1:], new):
                    dxa[0, a, :] = val
                own_dn[layer, st, rows, :] = new[0].astype(BF16)
            return 0

        lax.fori_loop(0, DOWN_ROWS // 16, body, 0)

    pairs_up = ((s_mas_up, o_mas_up), (s_mo_up, o_mo_up), (s_ve_up, o_ve_up))

    def out_copies(layer, mat):
        if mat == 0:
            return [pltpu.make_async_copy(src.at[:, layer], dst.at[:, layer], out_sem.at[layer, 0, i])
                    for i, (src, dst) in enumerate(pairs_up)]
        return [pltpu.make_async_copy(dn_view(layer, i + 1, st), dst.at[st, layer], out_sem.at[layer, 1 + st, i])
                for i, dst in enumerate((o_mas_dn, o_mo_dn, o_ve_dn)) for st in range(2)]

    def gather(layer, mat):
        if mat == 0:
            rows = pl.ds(pl.multiple_of(me * UP_ROWS, UP_ROWS), UP_ROWS)
            own, full = own_up, w1
        else:
            rows = pl.ds(pl.multiple_of(me * DOWN_ROWS, DOWN_ROWS), DOWN_ROWS)
            own, full = own_dn, w2

        def body(i, _):
            dest = lax.rem(me + i, NDEV)
            pltpu.make_async_remote_copy(
                src_ref=own.at[layer, lax.rem(dest, 2)], dst_ref=full.at[layer, rows, :],
                send_sem=ag_send.at[layer, mat], recv_sem=ag_recv.at[layer, mat],
                device_id=(dest,), device_id_type=MESH).start()
            return 0

        lax.fori_loop(1, NDEV, body, 0)
        full[layer, rows, :] = own[layer, stage]

    def ag_ref(layer, mat):
        if mat == 0:
            return w1.at[layer, pl.ds(0, D - UP_ROWS), :]
        return w2.at[layer, pl.ds(0, FF - DOWN_ROWS), :]

    def ag_wait(layer, mat):
        ref = ag_ref(layer, mat)
        pltpu.make_async_copy(ref, ref, ag_recv.at[layer, mat]).wait()

    rs_wait(1, 0)
    adam_up(1)
    rs_wait(1, 1)
    adam_dn(1)
    rs_wait(0, 0)
    adam_up(0)
    gather(0, 0)
    rs_wait(0, 1)
    adam_dn(0)
    gather(0, 1)
    gather(1, 0)
    gather(1, 1)
    for layer in range(2):
        for mat in range(2):
            for c in out_copies(layer, mat):
                c.start()
    own_next.wait()
    pushes[3].wait_recv()

    def forward(layer, src, dst, last):
        ag_wait(layer, 0)
        ag_wait(layer, 1)

        def body(b, _):
            q = b // 4
            rows = pl.ds(pl.multiple_of(lax.rem(b, 4) * TB, TB), TB)
            x = src[q, rows, :]
            hidden = dot_nn(x, w1[layer])
            u, s = gelu_half(hidden)
            act = (hidden * s).astype(BF16)
            dst[q, rows, :] = (x.astype(F32) + dot_nn(act, w2[layer])).astype(BF16)
            if last:
                @pl.when(q == 0)
                def _():
                    pltpu.make_async_copy(dst.at[0, rows, :], y_out.at[stage, 0, rows, :], y_sem.at[0]).start()

                @pl.when(q == 1)
                def _():
                    pltpu.make_async_remote_copy(src_ref=dst.at[1, rows, :], dst_ref=y_out.at[stage, 0, rows, :],
                                                 send_sem=y_sem.at[1], recv_sem=y_sem.at[2],
                                                 device_id=(partner,), device_id_type=MESH).start()
            return 0

        lax.fori_loop(0, 8, body, 0)

    forward(0, xs_top, xs_low, False)
    forward(1, xs_low, dyb, True)

    for i in range(3):
        pltpu.make_async_copy(dyb.at[0], dyb.at[0], y_sem.at[i]).wait()
    for i in range(1, 4):
        pushes[i].wait_send()
    for layer in range(2):
        for mat in range(2):
            ref = (recv_up if mat == 0 else recv_dn).at[layer, pl.ds(0, NDEV - 1)]
            pltpu.make_async_copy(ref, ref, rs_send.at[layer, mat]).wait()
            ref = ag_ref(layer, mat)
            pltpu.make_async_copy(ref, ref, ag_send.at[layer, mat]).wait()
            for c in out_copies(layer, mat):
                c.wait()


def solution(mesh):
    tok_spec = P(None, 'fsdp')
    layer_spec = P(None, None, 'fsdp')
    rep_spec = P()
    any_spec = pl.BlockSpec(memory_space=pl.ANY)
    up_state = (2, 2, UP_ROWS, FF)
    dn_state = (2, 2, DOWN_ROWS, D)
    sds = jax.ShapeDtypeStruct
    dma = pltpu.SemaphoreType.DMA

    call = pl.pallas_call(
        step_kernel,
        out_shape=(sds(up_state, F32), sds(dn_state, F32)) * 3 + (sds((2, 1, SEQ, D), BF16),),
        in_specs=[any_spec] * 13,
        out_specs=(any_spec,) * 7,
        scratch_shapes=[
            pltpu.VMEM((2, SEQ, D), BF16), pltpu.VMEM((2, SEQ, D), BF16), pltpu.VMEM((2, SEQ, D), BF16),
            pltpu.VMEM((2, SEQ, D), F32),
            pltpu.VMEM((2, D, FF), BF16), pltpu.VMEM((2, FF, D), BF16),
            pltpu.VMEM((2, NCHUNK, D, FC), BF16), pltpu.VMEM((2, NDEV, DOWN_ROWS, D), BF16),
            pltpu.VMEM((2, NDEV, NCHUNK, UP_ROWS, FC), BF16), pltpu.VMEM((2, NDEV, DOWN_ROWS, D), BF16),
        ] + [pltpu.VMEM(up_state, F32)] * 4 + [
            pltpu.VMEM((2, 2, UP_ROWS, FF), BF16), pltpu.VMEM((2, 2, DOWN_ROWS, D), BF16),
            pltpu.VMEM((D, FC), F32), pltpu.VMEM((FC, D), F32),
            dma((27,)), dma((4,)), dma((4,)), dma((2, 2)), dma((2, 2)), dma((2, 2)), dma((2, 2)),
            dma((2, 3, 3)), dma((3,)), pltpu.SemaphoreType.REGULAR,
        ],
        compiler_params=pltpu.CompilerParams(collective_id=0, has_side_effects=True, vmem_limit_bytes=67043328),
    )

    def device_step(*args):
        return call(*args)

    return jax.shard_map(device_step, mesh=mesh, in_specs=(layer_spec, tok_spec, tok_spec, rep_spec, rep_spec) + (layer_spec,) * 8,
                         out_specs=(layer_spec,) * 6 + (tok_spec,), check_vma=False)
```

```python
import jax
import jax.numpy as jnp
from jax import lax
from jax.experimental import pallas as pl
from jax.experimental.pallas import tpu as pltpu
from jax.sharding import PartitionSpec as P

LEARN_RATE = 0.005
BETA_ONE = 0.9
BETA_TWO = 0.95
ADAM_EPS = 1e-8
WEIGHT_DECAY = 0.1
MICROBATCHES = 2
ADAM_STEP = 2
CORR_ONE = 1.0 - BETA_ONE ** ADAM_STEP
CORR_TWO = 1.0 - BETA_TWO ** ADAM_STEP

GELU_A = 0.7978845608028654
GELU_B = 0.044715 * GELU_A

MESH = pl.DeviceIdType.MESH
BF16 = jnp.bfloat16
F32 = jnp.float32

NDEV = 16
SEQ = 2048
D = 512
FF = 2048
FC = 256
NCHUNK = FF // FC
UP_ROWS = D // NDEV
DOWN_ROWS = FF // NDEV
TB = 512


def dot_nn(a, b):
    return lax.dot_general(a, b, (((1,), (0,)), ((), ())), preferred_element_type=F32)


def dot_nt(a, b):
    return lax.dot_general(a, b, (((1,), (1,)), ((), ())), preferred_element_type=F32)


def dot_tn(a, b):
    return lax.dot_general(a, b, (((0,), (0,)), ((), ())), preferred_element_type=F32)


def gelu_half(h):
    u = h * h
    return u, 0.5 * jnp.tanh(h * (GELU_B * u + GELU_A)) + 0.5


def gelu_and_grad(h, grad_act):
    u, s = gelu_half(h)
    g = h * s
    slope = s + (g - g * s) * ((6.0 * GELU_B) * u + 2.0 * GELU_A)
    return g.astype(BF16), (grad_act * slope).astype(BF16)


def adam_math(grad_sum, acc, master, mom, vel):
    grad_mean = (acc + grad_sum) / MICROBATCHES
    mom = BETA_ONE * mom + (1.0 - BETA_ONE) * grad_mean
    vel = BETA_TWO * vel + (1.0 - BETA_TWO) * grad_mean * grad_mean
    step_dir = (mom / CORR_ONE) / (jnp.sqrt(vel / CORR_TWO) + ADAM_EPS)
    master = master - LEARN_RATE * (step_dir + WEIGHT_DECAY * master)
    return master, mom, vel


def step_kernel(x_saved, grad_out, x_next, w_up, w_down, acc_up, acc_dn, mas_up, mas_dn, mo_up, mo_dn, ve_up, ve_dn,
                o_mas_up, o_mas_dn, o_mo_up, o_mo_dn, o_ve_up, o_ve_dn, y_out,
                xs_top, xs_low, dyb, dxa, w1, w2, sent_up, sent_dn, recv_up, recv_dn,
                s_acc_up, s_mas_up, s_mo_up, s_ve_up,
                own_up, own_dn, acc1, acc2,
                load_sem, tok_send, tok_recv, rs_send, rs_recv, ag_send, ag_recv, out_sem, y_sem, free_sem):
    me = lax.axis_index('fsdp')
    stage = lax.rem(me, 2)
    other = 1 - stage
    chip = me // 2
    partner = me + 1 - 2 * stage

    bits = (lax.rem(chip, 2), lax.rem(chip // 2, 2), chip // 4)

    def chip_xor(mask):
        flips = (lax.rem(mask, 2), lax.rem(mask // 2, 2), mask // 4)
        return sum(lax.rem(b + f, 2) * w for b, f, w in zip(bits, flips, (1, 2, 4)))

    def chip_at(mask):
        return sum(((1 - b) if mask & w else b) * w for b, w in zip(bits, (1, 2, 4)))

    def load(i, src, dst):
        return pltpu.make_async_copy(src, dst, load_sem.at[i])

    loads = [
        load(0, w_up.at[stage, 1], w1.at[1]),
        load(1, x_saved.at[stage, 1, 0], xs_top.at[0]),
        load(2, w_down.at[stage, 1], w2.at[1]),
        load(3, grad_out.at[stage, 0], dyb.at[0]),
        load(4, w_up.at[stage, 0], w1.at[0]),
        load(5, x_saved.at[stage, 0, 0], xs_low.at[0]),
        load(6, w_down.at[stage, 0], w2.at[0]),
        load(7, acc_up, s_acc_up), load(8, mas_up, s_mas_up), load(9, mo_up, s_mo_up), load(10, ve_up, s_ve_up),
    ]

    def dn_rows(layer, arr, st):
        return ((layer * 4 + arr) * 2 + st) * DOWN_ROWS

    def dn_view(layer, arr, st):
        return dxa.at[0, pl.ds(dn_rows(layer, arr, st), DOWN_ROWS), :]

    dn_loads = [load(11 + arr * 4 + layer * 2 + st, src.at[st, layer], dn_view(layer, arr, st))
                for arr, src in enumerate((acc_dn, mas_dn, mo_dn, ve_dn)) for layer in range(2) for st in range(2)]
    for c in loads[:4]:
        c.start()

    barrier = pltpu.get_barrier_semaphore()

    def greet(t, _):
        pl.semaphore_signal(barrier, inc=1, device_id=(lax.rem(me + t, NDEV),), device_id_type=MESH)
        return 0

    lax.fori_loop(1, NDEV, greet, 0)
    pl.semaphore_wait(barrier, NDEV - 1)

    def push(i, src, dst):
        return pltpu.make_async_remote_copy(src_ref=src, dst_ref=dst, send_sem=tok_send.at[i], recv_sem=tok_recv.at[i],
                                            device_id=(partner,), device_id_type=MESH)

    pushes = [
        push(0, x_saved.at[other, 1, 0], xs_top.at[1]),
        push(1, grad_out.at[other, 0], dyb.at[1]),
        push(2, x_saved.at[other, 0, 0], xs_low.at[1]),
        push(3, x_next.at[other, 0], xs_top.at[1]),
    ]
    for c in pushes[:3]:
        c.start()
    for c in loads[4:]:
        c.start()
    for c in loads[:4]:
        c.wait()

    def send_up(layer, chunk, dest):
        return pltpu.make_async_remote_copy(
            src_ref=sent_up.at[layer, chunk, pl.ds(pl.multiple_of(dest * UP_ROWS, UP_ROWS), UP_ROWS), :],
            dst_ref=recv_up.at[layer, me, chunk],
            send_sem=rs_send.at[layer, 0], recv_sem=rs_recv.at[layer, 0],
            device_id=(dest,), device_id_type=MESH)

    def send_dn(layer, chunk, core):
        dest = 2 * chunk + core
        return pltpu.make_async_remote_copy(
            src_ref=sent_dn.at[layer, dest],
            dst_ref=recv_dn.at[layer, me],
            send_sem=rs_send.at[layer, 1], recv_sem=rs_recv.at[layer, 1],
            device_id=(dest,), device_id_type=MESH)

    def backward(layer, xs, with_dx, first_waits):
        def chunk_body(t, _):
            chunk = chip_xor(NCHUNK - 1 - t)
            cols = pl.ds(pl.multiple_of(chunk * FC, FC), FC)

            def token_body(q, _):
                @pl.when(jnp.logical_and(t == 0, q == 1))
                def _():
                    for c in first_waits:
                        c.wait_recv()

                @pl.when(q == 0)
                def _():
                    acc1[...] = jnp.zeros_like(acc1)
                    acc2[...] = jnp.zeros_like(acc2)

                x = xs[q]
                dy = dyb[q]
                hidden = dot_nn(x, w1[layer, :, cols])
                grad_act = dot_nt(dy, w2[layer, cols, :])
                act, grad_hidden = gelu_and_grad(hidden, grad_act)
                acc2[...] += dot_tn(act, dy)
                acc1[...] += dot_tn(x, grad_hidden)
                if with_dx:
                    part = dot_nt(grad_hidden, w1[layer, :, cols])

                    @pl.when(t == 0)
                    def _():
                        dxa[q] = part

                    @pl.when(t > 0)
                    def _():
                        dxa[q] += part
                return 0

            lax.fori_loop(0, 2, token_body, 0)
            sent_up[layer, chunk] = acc1[...].astype(BF16)
            for core in range(2):
                sent_dn[layer, 2 * chunk + core] = acc2[core * DOWN_ROWS:(core + 1) * DOWN_ROWS, :].astype(BF16)

            @pl.when(t < NCHUNK - 1)
            def _():
                send_dn(layer, chunk, 0).start()
                send_dn(layer, chunk, 1).start()

            @pl.when(t == NCHUNK - 1)
            def _():
                send_dn(layer, chunk, other).start()
                recv_dn[layer, me] = sent_dn[layer, me]

            def send_body(i, _):
                send_up(layer, chunk, 2 * chip_xor((NDEV - i) // 2) + lax.rem(stage + NDEV - i, 2)).start()
                return 0

            lax.fori_loop(1, NDEV, send_body, 0)
            recv_up[layer, me, chunk] = sent_up[layer, chunk, pl.ds(pl.multiple_of(me * UP_ROWS, UP_ROWS), UP_ROWS), :]
            return 0

        lax.fori_loop(0, NCHUNK, chunk_body, 0)

    backward(1, xs_top, True, pushes[:2])
    pl.semaphore_signal(free_sem, inc=1, device_id=(partner,), device_id_type=MESH)

    def cot_body(b, _):
        q = b // 4
        rows = pl.ds(pl.multiple_of(lax.rem(b, 4) * TB, TB), TB)
        dyb[q, rows, :] = (dyb[q, rows, :].astype(F32) + dxa[q, rows, :]).astype(BF16)
        return 0

    lax.fori_loop(0, 8, cot_body, 0)
    for c in dn_loads:
        c.start()
    for c in loads[4:7]:
        c.wait()
    backward(0, xs_low, False, pushes[2:3])

    own_next = load(1, x_next.at[stage, 0], xs_top.at[0])
    own_next.start()
    pl.semaphore_wait(free_sem, 1)
    pushes[0].wait_send()
    pushes[3].start()
    for c in loads[7:] + dn_loads:
        c.wait()

    def rs_wait(layer, mat):
        ref = (recv_up if mat == 0 else recv_dn).at[layer, pl.ds(0, NDEV - 1)]
        pltpu.make_async_copy(ref, ref, rs_recv.at[layer, mat]).wait()

    def adam_up(layer):
        def body(chunk, _):
            cols = pl.ds(pl.multiple_of(chunk * FC, FC), FC)
            for st in range(2):
                total = recv_up[layer, st, chunk].astype(F32)
                for k in range(1, 8):
                    total = total + recv_up[layer, 2 * k + st, chunk].astype(F32)
                new = adam_math(total, s_acc_up[st, layer, :, cols], s_mas_up[st, layer, :, cols],
                                s_mo_up[st, layer, :, cols], s_ve_up[st, layer, :, cols])
                s_mas_up[st, layer, :, cols] = new[0]
                s_mo_up[st, layer, :, cols] = new[1]
                s_ve_up[st, layer, :, cols] = new[2]
                own_up[layer, st, :, cols] = new[0].astype(BF16)
            return 0

        lax.fori_loop(0, NCHUNK, body, 0)

    def adam_dn(layer):
        def body(r, _):
            rows = pl.ds(pl.multiple_of(r * 16, 16), 16)
            for st in range(2):
                total = recv_dn[layer, st, rows, :].astype(F32)
                for k in range(1, 8):
                    total = total + recv_dn[layer, 2 * k + st, rows, :].astype(F32)
                at = [pl.ds(pl.multiple_of(dn_rows(layer, arr, st) + r * 16, 16), 16) for arr in range(4)]
                new = adam_math(total, *(dxa[0, a, :] for a in at))
                for a, val in zip(at[1:], new):
                    dxa[0, a, :] = val
                own_dn[layer, st, rows, :] = new[0].astype(BF16)
            return 0

        lax.fori_loop(0, DOWN_ROWS // 16, body, 0)

    pairs_up = ((s_mas_up, o_mas_up), (s_mo_up, o_mo_up), (s_ve_up, o_ve_up))

    def out_copies(layer, mat):
        if mat == 0:
            return [pltpu.make_async_copy(src.at[:, layer], dst.at[:, layer], out_sem.at[layer, 0, i])
                    for i, (src, dst) in enumerate(pairs_up)]
        return [pltpu.make_async_copy(dn_view(layer, i + 1, st), dst.at[st, layer], out_sem.at[layer, 1 + st, i])
                for i, dst in enumerate((o_mas_dn, o_mo_dn, o_ve_dn)) for st in range(2)]

    def piece_rows(layer, mat, dev):
        if mat == 0:
            return w1.at[layer, pl.ds(pl.multiple_of(dev * UP_ROWS, UP_ROWS), UP_ROWS), :]
        return w2.at[layer, pl.ds(pl.multiple_of(dev * DOWN_ROWS, DOWN_ROWS), DOWN_ROWS), :]

    def unit_rows(layer, mat, owner, part=None):
        full, size, cuts = ((w1, 2 * UP_ROWS, (0, 32, 48, 64)), (w2, 2 * DOWN_ROWS, (0, 96, 176, 256)))[mat]
        lo, hi = (0, size) if part is None else cuts[part:part + 2]
        return full.at[layer, pl.ds(pl.multiple_of(owner * size + lo, 16), hi - lo), :]

    def ag_copy(layer, mat, src, dst, slot, dest):
        return pltpu.make_async_remote_copy(src_ref=src, dst_ref=dst, send_sem=ag_send.at[layer, mat],
                                            recv_sem=ag_recv.at[layer, mat, slot],
                                            device_id=(dest,), device_id_type=MESH)

    def ag_got(layer, mat, slot, ref):
        pltpu.make_async_copy(ref, ref, ag_recv.at[layer, mat, slot]).wait()

    def round0(layer, mat):
        own = (own_up, own_dn)[mat]
        ag_copy(layer, mat, own.at[layer, other], piece_rows(layer, mat, me), 0, partner).start()
        piece_rows(layer, mat, me)[...] = own[layer, stage]

    def neighbour(mask):
        return 2 * chip_at(mask) + stage

    def send_unit(layer, mat, owner, slot, mask, part=None):
        ref = unit_rows(layer, mat, chip_at(owner), part)
        ag_copy(layer, mat, ref, ref, slot, neighbour(mask)).start()

    def round1(layer, mat):
        ag_got(layer, mat, 0, piece_rows(layer, mat, partner))
        for i in range(3):
            send_unit(layer, mat, 0, 1 + i, 1 << i)

    def round2(layer, mat):
        for link, came in ((0, 1), (1, 2), (2, 0)):
            ag_got(layer, mat, 1 + came, unit_rows(layer, mat, chip_at(1 << came)))
            send_unit(layer, mat, 1 << came, 4 + link, 1 << link)

    def round3(layer, mat):
        for link, owner, came in ((2, 3, 0), (0, 6, 1), (1, 5, 2)):
            ag_got(layer, mat, 4 + came, unit_rows(layer, mat, chip_at(owner)))
            send_unit(layer, mat, owner, 7, 1 << link, link)

    def ag_ref(layer, mat):
        if mat == 0:
            return w1.at[layer, pl.ds(0, D - UP_ROWS), :]
        return w2.at[layer, pl.ds(0, FF - DOWN_ROWS), :]

    def ag_wait(layer, mat):
        ag_got(layer, mat, 7, unit_rows(layer, mat, chip_at(7)))

    rs_wait(1, 0)
    adam_up(1)
    rs_wait(1, 1)
    adam_dn(1)
    rs_wait(0, 0)
    adam_up(0)
    round0(0, 0)
    rs_wait(0, 1)
    adam_dn(0)
    round0(0, 1)
    round1(0, 0)
    round1(0, 1)
    round0(1, 0)
    round0(1, 1)
    round2(0, 0)
    round2(0, 1)
    round3(0, 0)
    round1(1, 0)
    round3(0, 1)
    round1(1, 1)
    for layer in range(2):
        for mat in range(2):
            for c in out_copies(layer, mat):
                c.start()
    own_next.wait()
    pushes[3].wait_recv()

    def forward(layer, src, dst, last):
        ag_wait(layer, 0)
        ag_wait(layer, 1)

        def body(b, _):
            q = b // 4
            rows = pl.ds(pl.multiple_of(lax.rem(b, 4) * TB, TB), TB)
            x = src[q, rows, :]
            hidden = dot_nn(x, w1[layer])
            u, s = gelu_half(hidden)
            act = (hidden * s).astype(BF16)
            dst[q, rows, :] = (x.astype(F32) + dot_nn(act, w2[layer])).astype(BF16)
            if not last:
                for at, step, mat in ((1, round2, 0), (3, round2, 1), (5, round3, 0), (7, round3, 1)):
                    @pl.when(b == at)
                    def _(step=step, mat=mat):
                        step(1, mat)
            if last:
                @pl.when(q == 0)
                def _():
                    pltpu.make_async_copy(dst.at[0, rows, :], y_out.at[stage, 0, rows, :], y_sem.at[0]).start()

                @pl.when(q == 1)
                def _():
                    pltpu.make_async_remote_copy(src_ref=dst.at[1, rows, :], dst_ref=y_out.at[stage, 0, rows, :],
                                                 send_sem=y_sem.at[1], recv_sem=y_sem.at[2],
                                                 device_id=(partner,), device_id_type=MESH).start()
            return 0

        lax.fori_loop(0, 8, body, 0)

    forward(0, xs_top, xs_low, False)
    forward(1, xs_low, dyb, True)

    for i in range(3):
        pltpu.make_async_copy(dyb.at[0], dyb.at[0], y_sem.at[i]).wait()
    for i in range(1, 4):
        pushes[i].wait_send()
    for layer in range(2):
        for mat in range(2):
            ref = (recv_up if mat == 0 else recv_dn).at[layer, pl.ds(0, NDEV - 1)]
            pltpu.make_async_copy(ref, ref, rs_send.at[layer, mat]).wait()
            ref = ag_ref(layer, mat)
            pltpu.make_async_copy(ref, ref, ag_send.at[layer, mat]).wait()
            for c in out_copies(layer, mat):
                c.wait()


def solution(mesh):
    tok_spec = P(None, 'fsdp')
    layer_spec = P(None, None, 'fsdp')
    rep_spec = P()
    any_spec = pl.BlockSpec(memory_space=pl.ANY)
    up_state = (2, 2, UP_ROWS, FF)
    dn_state = (2, 2, DOWN_ROWS, D)
    sds = jax.ShapeDtypeStruct
    dma = pltpu.SemaphoreType.DMA

    call = pl.pallas_call(
        step_kernel,
        out_shape=(sds(up_state, F32), sds(dn_state, F32)) * 3 + (sds((2, 1, SEQ, D), BF16),),
        in_specs=[any_spec] * 13,
        out_specs=(any_spec,) * 7,
        scratch_shapes=[
            pltpu.VMEM((2, SEQ, D), BF16), pltpu.VMEM((2, SEQ, D), BF16), pltpu.VMEM((2, SEQ, D), BF16),
            pltpu.VMEM((2, SEQ, D), F32),
            pltpu.VMEM((2, D, FF), BF16), pltpu.VMEM((2, FF, D), BF16),
            pltpu.VMEM((2, NCHUNK, D, FC), BF16), pltpu.VMEM((2, NDEV, DOWN_ROWS, D), BF16),
            pltpu.VMEM((2, NDEV, NCHUNK, UP_ROWS, FC), BF16), pltpu.VMEM((2, NDEV, DOWN_ROWS, D), BF16),
        ] + [pltpu.VMEM(up_state, F32)] * 4 + [
            pltpu.VMEM((2, 2, UP_ROWS, FF), BF16), pltpu.VMEM((2, 2, DOWN_ROWS, D), BF16),
            pltpu.VMEM((D, FC), F32), pltpu.VMEM((FC, D), F32),
            dma((27,)), dma((4,)), dma((4,)), dma((2, 2)), dma((2, 2)), dma((2, 2)), dma((2, 2, 8)),
            dma((2, 3, 3)), dma((3,)), pltpu.SemaphoreType.REGULAR,
        ],
        compiler_params=pltpu.CompilerParams(collective_id=0, has_side_effects=True, vmem_limit_bytes=67043328),
    )

    def device_step(*args):
        return call(*args)

    return jax.shard_map(device_step, mesh=mesh, in_specs=(layer_spec, tok_spec, tok_spec, rep_spec, rep_spec) + (layer_spec,) * 8,
                         out_specs=(layer_spec,) * 6 + (tok_spec,), check_vma=False)
```

```python
import jax
import jax.numpy as jnp
from jax import lax
from jax.experimental import pallas as pl
from jax.experimental.pallas import tpu as pltpu
from jax.sharding import PartitionSpec as P

LEARN_RATE = 0.005
BETA_ONE = 0.9
BETA_TWO = 0.95
ADAM_EPS = 1e-8
WEIGHT_DECAY = 0.1
MICROBATCHES = 2
ADAM_STEP = 2
CORR_ONE = 1.0 - BETA_ONE ** ADAM_STEP
CORR_TWO = 1.0 - BETA_TWO ** ADAM_STEP

GELU_A = 0.7978845608028654
GELU_B = 0.044715 * GELU_A

MESH = pl.DeviceIdType.MESH
BF16 = jnp.bfloat16
F32 = jnp.float32

NDEV = 16
SEQ = 2048
D = 512
FF = 2048
FC = 256
NCHUNK = FF // FC
UP_ROWS = D // NDEV
DOWN_ROWS = FF // NDEV
TB = 1024
SUB = 1024
ARRIVAL = (0, 1, 2, 4, 3, 6, 5, 7)
ORDER = (7, 6, 5, 3, 1, 2, 4, 0)


def PRE(r1, r2, r3):
    return [(r1, 1, 0)]


def MID(r1, r2, r3):
    return [(r2, 0, 0), (r1, 0, 1), (r3, 0, 0)]


def BEFORE1A(r1, r2, r3):
    return [(r2, 0, 1)]


def HOOKS1A(r1, r2, r3):
    return {1: [(r2, 1, 0)], 2: [(r3, 0, 1)]}


def HOOKS1B(r1, r2, r3):
    return {1: [(r1, 1, 1)], 2: [(r3, 1, 0)]}


def BEFORE2A(r1, r2, r3):
    return [(r2, 1, 1)]


def HOOKS2A(r1, r2, r3):
    return {3: [(r3, 1, 1)]}


def dot_nn(a, b):
    return lax.dot_general(a, b, (((1,), (0,)), ((), ())), preferred_element_type=F32)


def dot_nt(a, b):
    return lax.dot_general(a, b, (((1,), (1,)), ((), ())), preferred_element_type=F32)


def dot_tn(a, b):
    return lax.dot_general(a, b, (((0,), (0,)), ((), ())), preferred_element_type=F32)


def gelu_half(h):
    u = h * h
    return u, 0.5 * jnp.tanh(h * (GELU_B * u + GELU_A)) + 0.5


def gelu_and_grad(h, grad_act):
    u, s = gelu_half(h)
    g = h * s
    slope = s + (g - g * s) * ((6.0 * GELU_B) * u + 2.0 * GELU_A)
    return g.astype(BF16), (grad_act * slope).astype(BF16)


def adam_math(grad_sum, acc, master, mom, vel):
    grad_mean = (acc + grad_sum) / MICROBATCHES
    mom = BETA_ONE * mom + (1.0 - BETA_ONE) * grad_mean
    vel = BETA_TWO * vel + (1.0 - BETA_TWO) * grad_mean * grad_mean
    step_dir = (mom / CORR_ONE) / (jnp.sqrt(vel / CORR_TWO) + ADAM_EPS)
    master = master - LEARN_RATE * (step_dir + WEIGHT_DECAY * master)
    return master, mom, vel


def step_kernel(x_saved, grad_out, x_next, w_up, w_down, acc_up, acc_dn, mas_up, mas_dn, mo_up, mo_dn, ve_up, ve_dn,
                o_mas_up, o_mas_dn, o_mo_up, o_mo_dn, o_ve_up, o_ve_dn, y_out,
                xs_top, xs_low, dyb, dxa, w1, w2, sent_up, sent_dn, recv_up, recv_dn,
                s_acc_up, s_mas_up, s_mo_up, s_ve_up,
                own_up, own_dn, acc1, acc2, act_buf, dh_buf,
                load_sem, tok_send, tok_recv, rs_send, rs_recv, ag_send, ag_recv, out_sem, y_sem, free_sem):
    me = lax.axis_index('fsdp')
    stage = lax.rem(me, 2)
    other = 1 - stage
    chip = me // 2
    partner = me + 1 - 2 * stage

    bits = (lax.rem(chip, 2), lax.rem(chip // 2, 2), chip // 4)

    def chip_xor(mask):
        flips = (lax.rem(mask, 2), lax.rem(mask // 2, 2), mask // 4)
        return sum(lax.rem(b + f, 2) * w for b, f, w in zip(bits, flips, (1, 2, 4)))

    def pick(table, i):
        return sum(jnp.where(i == k, v, 0) for k, v in enumerate(table))

    def chip_at(mask):
        return sum(((1 - b) if mask & w else b) * w for b, w in zip(bits, (1, 2, 4)))

    def load(i, src, dst):
        return pltpu.make_async_copy(src, dst, load_sem.at[i])

    loads = [
        load(0, w_up.at[stage, 1], w1.at[1]),
        load(1, x_saved.at[stage, 1, 0], xs_top.at[0]),
        load(2, w_down.at[stage, 1], w2.at[1]),
        load(3, grad_out.at[stage, 0], dyb.at[0]),
        load(4, w_up.at[stage, 0], w1.at[0]),
        load(5, x_saved.at[stage, 0, 0], xs_low.at[0]),
        load(6, w_down.at[stage, 0], w2.at[0]),
        load(7, acc_up, s_acc_up), load(8, mas_up, s_mas_up), load(9, mo_up, s_mo_up), load(10, ve_up, s_ve_up),
    ]

    def dn_rows(layer, arr, st):
        return ((layer * 4 + arr) * 2 + st) * DOWN_ROWS

    def dn_view(layer, arr, st):
        return dxa.at[0, pl.ds(dn_rows(layer, arr, st), DOWN_ROWS), :]

    dn_loads = [load(11 + arr * 4 + layer * 2 + st, src.at[st, layer], dn_view(layer, arr, st))
                for arr, src in enumerate((acc_dn, mas_dn, mo_dn, ve_dn)) for layer in range(2) for st in range(2)]
    for c in loads[:4]:
        c.start()

    barrier = pltpu.get_barrier_semaphore()

    def greet(t, _):
        pl.semaphore_signal(barrier, inc=1, device_id=(lax.rem(me + t, NDEV),), device_id_type=MESH)
        return 0

    lax.fori_loop(1, NDEV, greet, 0)
    pl.semaphore_wait(barrier, NDEV - 1)

    def push(i, src, dst):
        return pltpu.make_async_remote_copy(src_ref=src, dst_ref=dst, send_sem=tok_send.at[i], recv_sem=tok_recv.at[i],
                                            device_id=(partner,), device_id_type=MESH)

    pushes = [
        push(0, x_saved.at[other, 1, 0], xs_top.at[1]),
        push(1, grad_out.at[other, 0], dyb.at[1]),
        push(2, x_saved.at[other, 0, 0], xs_low.at[1]),
        push(3, x_next.at[other, 0], xs_top.at[1]),
    ]
    for c in pushes[:3]:
        c.start()
    for c in loads[4:]:
        c.start()
    for c in loads[:4]:
        c.wait()

    def down_rows(dev):
        return pl.ds(pl.multiple_of(dev * DOWN_ROWS, DOWN_ROWS), DOWN_ROWS)

    def send_up(layer, chunk, dest):
        return pltpu.make_async_remote_copy(
            src_ref=sent_up.at[layer, chunk, pl.ds(pl.multiple_of(dest * UP_ROWS, UP_ROWS), UP_ROWS), :],
            dst_ref=recv_up.at[layer, chunk, pl.ds(pl.multiple_of(me * UP_ROWS, UP_ROWS), UP_ROWS), :],
            send_sem=rs_send.at[layer, 0], recv_sem=rs_recv.at[layer, 0],
            device_id=(dest,), device_id_type=MESH)

    def send_dn(layer, chunk, core):
        dest = 2 * chunk + core
        return pltpu.make_async_remote_copy(
            src_ref=sent_dn.at[layer, down_rows(dest), :],
            dst_ref=recv_dn.at[layer, down_rows(me), :],
            send_sem=rs_send.at[layer, 1], recv_sem=rs_recv.at[layer, 1],
            device_id=(dest,), device_id_type=MESH)

    up_dests = [2 * chip_at(m) + core for m in ORDER[:-1] for core in range(2)] + [partner]

    def backward(layer, xs, with_dx, first_waits):
        def chunk_body(t, _):
            chunk = chip_xor(pick(ORDER, t))
            cols = pl.ds(pl.multiple_of(chunk * FC, FC), FC)

            def token_body(q, _):
                @pl.when(jnp.logical_and(t == 0, q == 1))
                def _():
                    for c in first_waits:
                        c.wait_recv()

                @pl.when(q == 0)
                def _():
                    acc1[...] = jnp.zeros_like(acc1)
                    acc2[...] = jnp.zeros_like(acc2)

                x = xs[q]
                dy = dyb[q]
                for lo in range(0, SEQ, SUB):
                    part_rows = slice(lo, lo + SUB)
                    hidden = dot_nn(x[part_rows], w1[layer, :, cols])
                    grad_act = dot_nt(dy[part_rows], w2[layer, cols, :])
                    act_buf[part_rows, :], dh_buf[part_rows, :] = gelu_and_grad(hidden, grad_act)
                act = act_buf[...]
                grad_hidden = dh_buf[...]
                acc2[...] += dot_tn(act, dy)
                acc1[...] += dot_tn(x, grad_hidden)
                if with_dx:
                    part = dot_nt(grad_hidden, w1[layer, :, cols])

                    @pl.when(t == 0)
                    def _():
                        dxa[q] = part

                    @pl.when(t > 0)
                    def _():
                        dxa[q] += part
                return 0

            lax.fori_loop(0, 2, token_body, 0)
            sent_up[layer, chunk] = acc1[...].astype(BF16)
            sent_dn[layer, cols, :] = acc2[...].astype(BF16)

            @pl.when(t < NCHUNK - 1)
            def _():
                send_dn(layer, chunk, 0).start()
                send_dn(layer, chunk, 1).start()

            @pl.when(t == NCHUNK - 1)
            def _():
                send_dn(layer, chunk, other).start()
                recv_dn[layer, down_rows(me), :] = sent_dn[layer, down_rows(me), :]

            for dest in up_dests:
                send_up(layer, chunk, dest).start()
            own_rows = pl.ds(pl.multiple_of(me * UP_ROWS, UP_ROWS), UP_ROWS)
            recv_up[layer, chunk, own_rows, :] = sent_up[layer, chunk, own_rows, :]
            return 0

        lax.fori_loop(0, NCHUNK, chunk_body, 0)

    backward(1, xs_top, True, pushes[:2])
    pl.semaphore_signal(free_sem, inc=1, device_id=(partner,), device_id_type=MESH)

    def token_rows(b):
        return b // 2, pl.ds(pl.multiple_of(lax.rem(b, 2) * TB, TB), TB)

    def cot_body(b, _):
        q, rows = token_rows(b)
        dyb[q, rows, :] = (dyb[q, rows, :].astype(F32) + dxa[q, rows, :]).astype(BF16)
        return 0

    lax.fori_loop(0, 4, cot_body, 0)
    for c in dn_loads:
        c.start()
    for c in loads[4:7]:
        c.wait()
    backward(0, xs_low, False, pushes[2:3])

    own_next = load(1, x_next.at[stage, 0], xs_top.at[0])
    own_next.start()
    pl.semaphore_wait(free_sem, 1)
    pushes[0].wait_send()
    pushes[3].start()
    for c in loads[7:] + dn_loads:
        c.wait()

    def rs_ref(layer, mat):
        if mat == 0:
            return recv_up.at[layer, :, pl.ds(0, D - UP_ROWS), :]
        return recv_dn.at[layer, pl.ds(0, FF - DOWN_ROWS), :]

    def rs_wait(layer, mat):
        ref = rs_ref(layer, mat)
        pltpu.make_async_copy(ref, ref, rs_recv.at[layer, mat]).wait()

    def adam_up(layer):
        def body(chunk, _):
            cols = pl.ds(pl.multiple_of(chunk * FC, FC), FC)
            for st in range(2):
                total = recv_up[layer, chunk, pl.ds(st * UP_ROWS, UP_ROWS), :].astype(F32)
                for k in range(1, 8):
                    total = total + recv_up[layer, chunk, pl.ds((2 * k + st) * UP_ROWS, UP_ROWS), :].astype(F32)
                new = adam_math(total, s_acc_up[st, layer, :, cols], s_mas_up[st, layer, :, cols],
                                s_mo_up[st, layer, :, cols], s_ve_up[st, layer, :, cols])
                s_mas_up[st, layer, :, cols] = new[0]
                s_mo_up[st, layer, :, cols] = new[1]
                s_ve_up[st, layer, :, cols] = new[2]
                own_up[layer, st, :, cols] = new[0].astype(BF16)
            return 0

        lax.fori_loop(0, NCHUNK, body, 0)

    def adam_dn(layer):
        def body(r, _):
            rows = pl.ds(pl.multiple_of(r * 16, 16), 16)
            for st in range(2):
                from_dev = [pl.ds(pl.multiple_of((2 * k + st) * DOWN_ROWS + r * 16, 16), 16) for k in range(8)]
                total = recv_dn[layer, from_dev[0], :].astype(F32)
                for k in range(1, 8):
                    total = total + recv_dn[layer, from_dev[k], :].astype(F32)
                at = [pl.ds(pl.multiple_of(dn_rows(layer, arr, st) + r * 16, 16), 16) for arr in range(4)]
                new = adam_math(total, *(dxa[0, a, :] for a in at))
                for a, val in zip(at[1:], new):
                    dxa[0, a, :] = val
                own_dn[layer, st, rows, :] = new[0].astype(BF16)
            return 0

        lax.fori_loop(0, DOWN_ROWS // 16, body, 0)

    pairs_up = ((s_mas_up, o_mas_up), (s_mo_up, o_mo_up), (s_ve_up, o_ve_up))

    def out_copies(layer, mat):
        if mat == 0:
            return [pltpu.make_async_copy(src.at[:, layer], dst.at[:, layer], out_sem.at[layer, 0, i])
                    for i, (src, dst) in enumerate(pairs_up)]
        return [pltpu.make_async_copy(dn_view(layer, i + 1, st), dst.at[st, layer], out_sem.at[layer, 1 + st, i])
                for i, dst in enumerate((o_mas_dn, o_mo_dn, o_ve_dn)) for st in range(2)]

    def piece_rows(layer, mat, dev):
        if mat == 0:
            return w1.at[layer, pl.ds(pl.multiple_of(dev * UP_ROWS, UP_ROWS), UP_ROWS), :]
        return w2.at[layer, pl.ds(pl.multiple_of(dev * DOWN_ROWS, DOWN_ROWS), DOWN_ROWS), :]

    def unit_rows(layer, mat, owner, part=None):
        full, size, cuts = ((w1, 2 * UP_ROWS, (0, 32, 48, 64)), (w2, 2 * DOWN_ROWS, (0, 96, 176, 256)))[mat]
        lo, hi = (0, size) if part is None else cuts[part:part + 2]
        return full.at[layer, pl.ds(pl.multiple_of(owner * size + lo, 16), hi - lo), :]

    def ag_copy(layer, mat, src, dst, slot, dest):
        return pltpu.make_async_remote_copy(src_ref=src, dst_ref=dst, send_sem=ag_send.at[layer, mat],
                                            recv_sem=ag_recv.at[layer, mat, slot],
                                            device_id=(dest,), device_id_type=MESH)

    def ag_got(layer, mat, slot, ref):
        pltpu.make_async_copy(ref, ref, ag_recv.at[layer, mat, slot]).wait()

    def round0(layer, mat):
        own = (own_up, own_dn)[mat]
        ag_copy(layer, mat, own.at[layer, other], piece_rows(layer, mat, me), 0, partner).start()
        piece_rows(layer, mat, me)[...] = own[layer, stage]

    def neighbour(mask):
        return 2 * chip_at(mask) + stage

    def send_unit(layer, mat, owner, slot, mask, part=None):
        ref = unit_rows(layer, mat, chip_at(owner), part)
        ag_copy(layer, mat, ref, ref, slot, neighbour(mask)).start()

    def round1(layer, mat):
        ag_got(layer, mat, 0, piece_rows(layer, mat, partner))
        for i in range(3):
            send_unit(layer, mat, 0, 1 + i, 1 << i)

    def round2(layer, mat):
        for link, came in ((0, 1), (1, 2), (2, 0)):
            ag_got(layer, mat, 1 + came, unit_rows(layer, mat, chip_at(1 << came)))
            send_unit(layer, mat, 1 << came, 4 + link, 1 << link)

    def round3(layer, mat):
        for link, owner, came in ((2, 3, 0), (0, 6, 1), (1, 5, 2)):
            ag_got(layer, mat, 4 + came, unit_rows(layer, mat, chip_at(owner)))
            send_unit(layer, mat, owner, 7, 1 << link, link)

    def ag_ref(layer, mat):
        if mat == 0:
            return w1.at[layer, pl.ds(0, D - UP_ROWS), :]
        return w2.at[layer, pl.ds(0, FF - DOWN_ROWS), :]

    def ag_wait(layer, mat):
        ag_got(layer, mat, 7, unit_rows(layer, mat, chip_at(7)))

    def run(calls):
        for fn, *where in calls:
            fn(*where)

    def hooked(b, hooks):
        for at, calls in hooks.items():
            @pl.when(b == at)
            def _(calls=calls):
                run(calls)

    def feature_rows(pos):
        return pl.ds(pl.multiple_of(chip_at(ARRIVAL[pos]) * FC, FC), FC)

    def forward_pass(layer, src, dst, lo, hi, hooks):
        final = layer == 1 and hi == NCHUNK

        def body(b, _):
            hooked(b, hooks)
            q, rows = token_rows(b)
            x = src[q, rows, :]
            hidden = dot_nn(x, jnp.concatenate([w1[layer, :, feature_rows(pos)] for pos in range(lo, hi)], axis=1))
            u, s = gelu_half(hidden)
            part = dot_nn((hidden * s).astype(BF16),
                          jnp.concatenate([w2[layer, feature_rows(pos), :] for pos in range(lo, hi)], axis=0))
            if lo > 0:
                part = part + dxa[q, rows, :]
            if hi < NCHUNK:
                dxa[q, rows, :] = part
            else:
                dst[q, rows, :] = (x.astype(F32) + part).astype(BF16)
            if final:
                @pl.when(q == 0)
                def _():
                    pltpu.make_async_copy(dst.at[0, rows, :], y_out.at[stage, 0, rows, :], y_sem.at[0]).start()

                @pl.when(q == 1)
                def _():
                    pltpu.make_async_remote_copy(src_ref=dst.at[1, rows, :], dst_ref=y_out.at[stage, 0, rows, :],
                                                 send_sem=y_sem.at[1], recv_sem=y_sem.at[2],
                                                 device_id=(partner,), device_id_type=MESH).start()
            return 0

        lax.fori_loop(0, 4, body, 0)

    r1, r2, r3 = round1, round2, round3

    rs_wait(1, 0)
    adam_up(1)
    round0(1, 0)
    rs_wait(1, 1)
    adam_dn(1)
    round0(1, 1)
    run(PRE(r1, r2, r3))
    rs_wait(0, 0)
    adam_up(0)
    round0(0, 0)
    rs_wait(0, 1)
    round1(0, 0)
    adam_dn(0)
    round0(0, 1)
    for layer in range(2):
        for mat in range(2):
            for c in out_copies(layer, mat):
                c.start()
    run(MID(r1, r2, r3))
    own_next.wait()
    pushes[3].wait_recv()
    for layer in range(2):
        for c in out_copies(layer, 1):
            c.wait()
    ag_wait(0, 0)
    run(BEFORE1A(r1, r2, r3))
    forward_pass(0, xs_top, xs_low, 0, 4, HOOKS1A(r1, r2, r3))
    ag_wait(0, 1)
    forward_pass(0, xs_top, xs_low, 4, 8, HOOKS1B(r1, r2, r3))
    run(BEFORE2A(r1, r2, r3))
    ag_wait(1, 0)
    forward_pass(1, xs_low, dyb, 0, 4, HOOKS2A(r1, r2, r3))
    ag_wait(1, 1)
    forward_pass(1, xs_low, dyb, 4, 8, {})

    for i in range(3):
        pltpu.make_async_copy(dyb.at[0], dyb.at[0], y_sem.at[i]).wait()
    for i in range(1, 4):
        pushes[i].wait_send()
    for layer in range(2):
        for mat in range(2):
            ref = rs_ref(layer, mat)
            pltpu.make_async_copy(ref, ref, rs_send.at[layer, mat]).wait()
            ref = ag_ref(layer, mat)
            pltpu.make_async_copy(ref, ref, ag_send.at[layer, mat]).wait()
            if mat == 0:
                for c in out_copies(layer, mat):
                    c.wait()


def emit_kernel(*refs):
    src, dst, buf = refs[:7], refs[7:14], refs[14:21]
    in_sem, done_sem = refs[21:]
    spots = [(i, half) for i in range(7) for half in range(2)]
    into = [pltpu.make_async_copy(src[i].at[h], buf[i].at[h], in_sem.at[i, h]) for i, h in spots]
    out = [pltpu.make_async_copy(buf[i].at[h], dst[i].at[h], done_sem.at[i, h]) for i, h in spots]
    for c in into:
        c.start()
    for c, d in zip(into, out):
        c.wait()
        d.start()
    for d in out:
        d.wait()


def solution(mesh):
    tok_spec = P(None, 'fsdp')
    layer_spec = P(None, None, 'fsdp')
    rep_spec = P()
    any_spec = pl.BlockSpec(memory_space=pl.ANY)
    up_state = (2, 2, UP_ROWS, FF)
    dn_state = (2, 2, DOWN_ROWS, D)
    sds = jax.ShapeDtypeStruct
    dma = pltpu.SemaphoreType.DMA

    call = pl.pallas_call(
        step_kernel,
        out_shape=(sds(up_state, F32), sds(dn_state, F32)) * 3 + (sds((2, 1, SEQ, D), BF16),),
        in_specs=[any_spec] * 13,
        out_specs=(any_spec,) * 7,
        scratch_shapes=[
            pltpu.VMEM((2, SEQ, D), BF16), pltpu.VMEM((2, SEQ, D), BF16), pltpu.VMEM((2, SEQ, D), BF16),
            pltpu.VMEM((2, SEQ, D), F32),
            pltpu.VMEM((2, D, FF), BF16), pltpu.VMEM((2, FF, D), BF16),
            pltpu.VMEM((2, NCHUNK, D, FC), BF16), pltpu.VMEM((2, FF, D), BF16),
            pltpu.VMEM((2, NCHUNK, D, FC), BF16), pltpu.VMEM((2, FF, D), BF16),
        ] + [pltpu.VMEM(up_state, F32)] * 4 + [
            pltpu.VMEM((2, 2, UP_ROWS, FF), BF16), pltpu.VMEM((2, 2, DOWN_ROWS, D), BF16),
            pltpu.VMEM((D, FC), F32), pltpu.VMEM((FC, D), F32),
            pltpu.VMEM((SEQ, FC), BF16), pltpu.VMEM((SEQ, FC), BF16),
            dma((27,)), dma((4,)), dma((4,)), dma((2, 2)), dma((2, 2)), dma((2, 2)), dma((2, 2, 8)),
            dma((2, 3, 3)), dma((3,)), pltpu.SemaphoreType.REGULAR,
        ],
        compiler_params=pltpu.CompilerParams(collective_id=0, has_side_effects=True, vmem_limit_bytes=67043328),
    )

    emit = pl.pallas_call(
        emit_kernel,
        out_shape=(sds(up_state, F32), sds(dn_state, F32)) * 3 + (sds((2, 1, SEQ, D), BF16),),
        in_specs=[any_spec] * 7,
        out_specs=(any_spec,) * 7,
        scratch_shapes=[pltpu.VMEM(up_state, F32), pltpu.VMEM(dn_state, F32)] * 3 + [pltpu.VMEM((2, 1, SEQ, D), BF16)] + [
            dma((7, 2)), dma((7, 2))],
        compiler_params=pltpu.CompilerParams(vmem_limit_bytes=67043328),
    )

    def device_step(*args):
        return emit(*call(*args))

    return jax.shard_map(device_step, mesh=mesh, in_specs=(layer_spec, tok_spec, tok_spec, rep_spec, rep_spec) + (layer_spec,) * 8,
                         out_specs=(layer_spec,) * 6 + (tok_spec,), check_vma=False)
```

```python
import jax
import jax.numpy as jnp
from jax import lax
from jax.experimental import pallas as pl
from jax.experimental.pallas import tpu as pltpu
from jax.sharding import PartitionSpec as P

LEARN_RATE = 0.005
BETA_ONE = 0.9
BETA_TWO = 0.95
ADAM_EPS = 1e-8
WEIGHT_DECAY = 0.1
MICROBATCHES = 2
ADAM_STEP = 2
CORR_ONE = 1.0 - BETA_ONE ** ADAM_STEP
CORR_TWO = 1.0 - BETA_TWO ** ADAM_STEP

GELU_A = 0.7978845608028654
GELU_B = 0.044715 * GELU_A

MESH = pl.DeviceIdType.MESH
BF16 = jnp.bfloat16
F32 = jnp.float32

NDEV = 16
SEQ = 2048
D = 512
FF = 2048
FC = 256
NCHUNK = FF // FC
UP_ROWS = D // NDEV
DOWN_ROWS = FF // NDEV
TB = 1024
SUB = 1024
ARRIVAL = (0, 1, 2, 4, 3, 6, 5, 7)
ORDER = (7, 6, 5, 3, 1, 2, 4, 0)


def PRE(r1, r2, r3):
    return [(r1, 1, 0)]


def MID(r1, r2, r3):
    return [(r2, 0, 0), (r1, 0, 1), (r3, 0, 0)]


def BEFORE1A(r1, r2, r3):
    return [(r2, 0, 1)]


def HOOKS1A(r1, r2, r3):
    return {1: [(r2, 1, 0)], 2: [(r3, 0, 1)]}


def HOOKS1B(r1, r2, r3):
    return {1: [(r1, 1, 1)], 2: [(r3, 1, 0)]}


def BEFORE2A(r1, r2, r3):
    return [(r2, 1, 1)]


def HOOKS2A(r1, r2, r3):
    return {3: [(r3, 1, 1)]}


def dot_nn(a, b):
    return lax.dot_general(a, b, (((1,), (0,)), ((), ())), preferred_element_type=F32)


def dot_nt(a, b):
    return lax.dot_general(a, b, (((1,), (1,)), ((), ())), preferred_element_type=F32)


def dot_tn(a, b):
    return lax.dot_general(a, b, (((0,), (0,)), ((), ())), preferred_element_type=F32)


def gelu_half(h):
    u = h * h
    return u, 0.5 * jnp.tanh(h * (GELU_B * u + GELU_A)) + 0.5


def gelu_and_grad(h, grad_act):
    u, s = gelu_half(h)
    g = h * s
    slope = s + (g - g * s) * ((6.0 * GELU_B) * u + 2.0 * GELU_A)
    return g.astype(BF16), (grad_act * slope).astype(BF16)


def adam_math(grad_sum, acc, master, mom, vel):
    grad_mean = (acc + grad_sum) / MICROBATCHES
    mom = BETA_ONE * mom + (1.0 - BETA_ONE) * grad_mean
    vel = BETA_TWO * vel + (1.0 - BETA_TWO) * grad_mean * grad_mean
    step_dir = (mom / CORR_ONE) / (jnp.sqrt(vel / CORR_TWO) + ADAM_EPS)
    master = master - LEARN_RATE * (step_dir + WEIGHT_DECAY * master)
    return master, mom, vel


def step_kernel(x_saved, grad_out, x_next, w_up, w_down, acc_up, acc_dn, mas_up, mas_dn, mo_up, mo_dn, ve_up, ve_dn,
                o_mas_up, o_mas_dn, o_mo_up, o_mo_dn, o_ve_up, o_ve_dn, y_out,
                xs_top, xs_low, dyb, dxa, w1, w2, sent_up, sent_dn, recv_up, recv_dn,
                s_acc_up, s_mas_up, s_mo_up, s_ve_up,
                own_up, own_dn, acc1, acc2,
                load_sem, tok_send, tok_recv, rs_send, rs_recv, ag_send, ag_recv, out_sem, y_sem, free_sem):
    me = lax.axis_index('fsdp')
    stage = lax.rem(me, 2)
    other = 1 - stage
    chip = me // 2
    partner = me + 1 - 2 * stage

    bits = (lax.rem(chip, 2), lax.rem(chip // 2, 2), chip // 4)

    def chip_xor(mask):
        flips = (lax.rem(mask, 2), lax.rem(mask // 2, 2), mask // 4)
        return sum(lax.rem(b + f, 2) * w for b, f, w in zip(bits, flips, (1, 2, 4)))

    def pick(table, i):
        return sum(jnp.where(i == k, v, 0) for k, v in enumerate(table))

    def chip_at(mask):
        return sum(((1 - b) if mask & w else b) * w for b, w in zip(bits, (1, 2, 4)))

    def load(i, src, dst):
        return pltpu.make_async_copy(src, dst, load_sem.at[i])

    loads = [
        load(0, w_up.at[stage, 1], w1.at[1]),
        load(1, x_saved.at[stage, 1, 0], xs_top.at[0]),
        load(2, w_down.at[stage, 1], w2.at[1]),
        load(3, grad_out.at[stage, 0], dyb.at[0]),
        load(4, w_up.at[stage, 0], w1.at[0]),
        load(5, x_saved.at[stage, 0, 0], xs_low.at[0]),
        load(6, w_down.at[stage, 0], w2.at[0]),
        load(7, acc_up, s_acc_up), load(8, mas_up, s_mas_up), load(9, mo_up, s_mo_up), load(10, ve_up, s_ve_up),
    ]

    def dn_rows(layer, arr, st):
        return ((layer * 4 + arr) * 2 + st) * DOWN_ROWS

    def dn_view(layer, arr, st):
        return dxa.at[0, pl.ds(dn_rows(layer, arr, st), DOWN_ROWS), :]

    dn_loads = [load(11 + arr * 4 + layer * 2 + st, src.at[st, layer], dn_view(layer, arr, st))
                for arr, src in enumerate((acc_dn, mas_dn, mo_dn, ve_dn)) for layer in range(2) for st in range(2)]
    for c in loads[:4]:
        c.start()

    barrier = pltpu.get_barrier_semaphore()

    def greet(t, _):
        pl.semaphore_signal(barrier, inc=1, device_id=(lax.rem(me + t, NDEV),), device_id_type=MESH)
        return 0

    lax.fori_loop(1, NDEV, greet, 0)
    pl.semaphore_wait(barrier, NDEV - 1)

    def push(i, src, dst):
        return pltpu.make_async_remote_copy(src_ref=src, dst_ref=dst, send_sem=tok_send.at[i], recv_sem=tok_recv.at[i],
                                            device_id=(partner,), device_id_type=MESH)

    pushes = [
        push(0, x_saved.at[other, 1, 0], xs_top.at[1]),
        push(1, grad_out.at[other, 0], dyb.at[1]),
        push(2, x_saved.at[other, 0, 0], xs_low.at[1]),
        push(3, x_next.at[other, 0], xs_top.at[1]),
    ]
    for c in pushes[:3]:
        c.start()
    for c in loads[4:]:
        c.start()

    def zero_body(b, _):
        dxa[b // 4, pl.ds(pl.multiple_of(lax.rem(b, 4) * 512, 512), 512), :] = jnp.zeros((512, D), F32)
        return 0

    lax.fori_loop(0, 8, zero_body, 0)
    for c in loads[:4]:
        c.wait()

    def down_rows(dev):
        return pl.ds(pl.multiple_of(dev * DOWN_ROWS, DOWN_ROWS), DOWN_ROWS)

    def send_up(layer, chunk, dest):
        return pltpu.make_async_remote_copy(
            src_ref=sent_up.at[layer, chunk, pl.ds(pl.multiple_of(dest * UP_ROWS, UP_ROWS), UP_ROWS), :],
            dst_ref=recv_up.at[layer, chunk, pl.ds(pl.multiple_of(me * UP_ROWS, UP_ROWS), UP_ROWS), :],
            send_sem=rs_send.at[layer, 0], recv_sem=rs_recv.at[layer, 0],
            device_id=(dest,), device_id_type=MESH)

    def send_dn(layer, chunk, core):
        dest = 2 * chunk + core
        return pltpu.make_async_remote_copy(
            src_ref=sent_dn.at[layer, down_rows(dest), :],
            dst_ref=recv_dn.at[layer, down_rows(me), :],
            send_sem=rs_send.at[layer, 1], recv_sem=rs_recv.at[layer, 1],
            device_id=(dest,), device_id_type=MESH)

    up_dests = [2 * chip_at(m) + core for m in ORDER[:-1] for core in range(2)] + [partner]

    def backward(layer, xs, with_dx, first_waits):
        def chunk_body(t, _, peeled=False):
            chunk = chip_xor(pick(ORDER, t))
            cols = pl.ds(pl.multiple_of(chunk * FC, FC), FC)

            def token_body(q):
                if q == 1 and peeled:
                    for c in first_waits:
                        c.wait_recv()

                x = xs[q]
                dy = dyb[q]
                tmp = sent_dn.at[0] if layer == 1 else xs_top.at[0]
                for lo in range(0, SEQ, SUB):
                    part_rows = slice(lo, lo + SUB)
                    hidden = dot_nn(x[part_rows], w1[layer, :, cols])
                    grad_act = dot_nt(dy[part_rows], w2[layer, cols, :])
                    tmp[part_rows, :FC], tmp[part_rows, FC:] = gelu_and_grad(hidden, grad_act)
                act = tmp[:, :FC]
                grad_hidden = tmp[:, FC:]
                part_dn = dot_tn(act, dy)
                part_up = dot_tn(x, grad_hidden)
                if q == 0:
                    acc2[...] = part_dn
                    acc1[...] = part_up
                else:
                    sent_dn[layer, cols, :] = (acc2[...] + part_dn).astype(BF16)
                    sent_up[layer, chunk] = (acc1[...] + part_up).astype(BF16)
                if with_dx:
                    dxa[q] += dot_nt(grad_hidden, w1[layer, :, cols])

            token_body(0)
            token_body(1)

            @pl.when(t < NCHUNK - 1)
            def _():
                send_dn(layer, chunk, 0).start()
                send_dn(layer, chunk, 1).start()

            @pl.when(t == NCHUNK - 1)
            def _():
                send_dn(layer, chunk, other).start()
                recv_dn[layer, down_rows(me), :] = sent_dn[layer, down_rows(me), :]

            for dest in up_dests:
                send_up(layer, chunk, dest).start()
            own_rows = pl.ds(pl.multiple_of(me * UP_ROWS, UP_ROWS), UP_ROWS)
            recv_up[layer, chunk, own_rows, :] = sent_up[layer, chunk, own_rows, :]
            return 0

        if with_dx:
            chunk_body(0, 0, True)
        else:
            for c in first_waits:
                c.wait_recv()
        lax.fori_loop(1 if with_dx else 0, NCHUNK, chunk_body, 0)

    backward(1, xs_top, True, pushes[:2])
    pl.semaphore_signal(free_sem, inc=1, device_id=(partner,), device_id_type=MESH)

    def token_rows(b):
        return b // 2, pl.ds(pl.multiple_of(lax.rem(b, 2) * TB, TB), TB)

    def cot_body(b, _):
        q, rows = token_rows(b)
        dyb[q, rows, :] = (dyb[q, rows, :].astype(F32) + dxa[q, rows, :]).astype(BF16)
        return 0

    lax.fori_loop(0, 4, cot_body, 0)
    for c in dn_loads:
        c.start()
    for c in loads[4:7]:
        c.wait()
    backward(0, xs_low, False, pushes[2:3])

    own_next = load(1, x_next.at[stage, 0], xs_top.at[0])
    own_next.start()
    pl.semaphore_wait(free_sem, 1)
    pushes[0].wait_send()
    pushes[3].start()
    for c in loads[7:] + dn_loads:
        c.wait()

    def rs_ref(layer, mat):
        if mat == 0:
            return recv_up.at[layer, :, pl.ds(0, D - UP_ROWS), :]
        return recv_dn.at[layer, pl.ds(0, FF - DOWN_ROWS), :]

    def rs_wait(layer, mat):
        ref = rs_ref(layer, mat)
        pltpu.make_async_copy(ref, ref, rs_recv.at[layer, mat]).wait()

    def adam_up(layer):
        def body(chunk, _):
            cols = pl.ds(pl.multiple_of(chunk * FC, FC), FC)
            for st in range(2):
                total = recv_up[layer, chunk, pl.ds(st * UP_ROWS, UP_ROWS), :].astype(F32)
                for k in range(1, 8):
                    total = total + recv_up[layer, chunk, pl.ds((2 * k + st) * UP_ROWS, UP_ROWS), :].astype(F32)
                new = adam_math(total, s_acc_up[st, layer, :, cols], s_mas_up[st, layer, :, cols],
                                s_mo_up[st, layer, :, cols], s_ve_up[st, layer, :, cols])
                s_mas_up[st, layer, :, cols] = new[0]
                s_mo_up[st, layer, :, cols] = new[1]
                s_ve_up[st, layer, :, cols] = new[2]
                own_up[layer, st, :, cols] = new[0].astype(BF16)
            return 0

        lax.fori_loop(0, NCHUNK, body, 0)

    def adam_dn(layer):
        def body(r, _):
            rows = pl.ds(pl.multiple_of(r * 16, 16), 16)
            for st in range(2):
                from_dev = [pl.ds(pl.multiple_of((2 * k + st) * DOWN_ROWS + r * 16, 16), 16) for k in range(8)]
                total = recv_dn[layer, from_dev[0], :].astype(F32)
                for k in range(1, 8):
                    total = total + recv_dn[layer, from_dev[k], :].astype(F32)
                at = [pl.ds(pl.multiple_of(dn_rows(layer, arr, st) + r * 16, 16), 16) for arr in range(4)]
                new = adam_math(total, *(dxa[0, a, :] for a in at))
                for a, val in zip(at[1:], new):
                    dxa[0, a, :] = val
                own_dn[layer, st, rows, :] = new[0].astype(BF16)
            return 0

        lax.fori_loop(0, DOWN_ROWS // 16, body, 0)

    pairs_up = ((s_mas_up, o_mas_up), (s_mo_up, o_mo_up), (s_ve_up, o_ve_up))

    def out_copies(layer, mat):
        if mat == 0:
            return [pltpu.make_async_copy(src.at[:, layer], dst.at[:, layer], out_sem.at[layer, 0, i])
                    for i, (src, dst) in enumerate(pairs_up)]
        return [pltpu.make_async_copy(dn_view(layer, i + 1, st), dst.at[st, layer], out_sem.at[layer, 1 + st, i])
                for i, dst in enumerate((o_mas_dn, o_mo_dn, o_ve_dn)) for st in range(2)]

    def piece_rows(layer, mat, dev):
        if mat == 0:
            return w1.at[layer, pl.ds(pl.multiple_of(dev * UP_ROWS, UP_ROWS), UP_ROWS), :]
        return w2.at[layer, pl.ds(pl.multiple_of(dev * DOWN_ROWS, DOWN_ROWS), DOWN_ROWS), :]

    def unit_rows(layer, mat, owner, part=None):
        full, size, cuts = ((w1, 2 * UP_ROWS, (0, 32, 48, 64)), (w2, 2 * DOWN_ROWS, (0, 96, 176, 256)))[mat]
        lo, hi = (0, size) if part is None else cuts[part:part + 2]
        return full.at[layer, pl.ds(pl.multiple_of(owner * size + lo, 16), hi - lo), :]

    def ag_copy(layer, mat, src, dst, slot, dest):
        return pltpu.make_async_remote_copy(src_ref=src, dst_ref=dst, send_sem=ag_send.at[layer, mat],
                                            recv_sem=ag_recv.at[layer, mat, slot],
                                            device_id=(dest,), device_id_type=MESH)

    def ag_got(layer, mat, slot, ref):
        pltpu.make_async_copy(ref, ref, ag_recv.at[layer, mat, slot]).wait()

    def round0(layer, mat):
        own = (own_up, own_dn)[mat]
        ag_copy(layer, mat, own.at[layer, other], piece_rows(layer, mat, me), 0, partner).start()
        piece_rows(layer, mat, me)[...] = own[layer, stage]

    def neighbour(mask):
        return 2 * chip_at(mask) + stage

    def send_unit(layer, mat, owner, slot, mask, part=None):
        ref = unit_rows(layer, mat, chip_at(owner), part)
        ag_copy(layer, mat, ref, ref, slot, neighbour(mask)).start()

    def round1(layer, mat):
        ag_got(layer, mat, 0, piece_rows(layer, mat, partner))
        for i in range(3):
            send_unit(layer, mat, 0, 1 + i, 1 << i)

    def round2(layer, mat):
        for link, came in ((0, 1), (1, 2), (2, 0)):
            ag_got(layer, mat, 1 + came, unit_rows(layer, mat, chip_at(1 << came)))
            send_unit(layer, mat, 1 << came, 4 + link, 1 << link)

    def round3(layer, mat):
        for link, owner, came in ((2, 3, 0), (0, 6, 1), (1, 5, 2)):
            ag_got(layer, mat, 4 + came, unit_rows(layer, mat, chip_at(owner)))
            send_unit(layer, mat, owner, 7, 1 << link, link)

    def ag_ref(layer, mat):
        if mat == 0:
            return w1.at[layer, pl.ds(0, D - UP_ROWS), :]
        return w2.at[layer, pl.ds(0, FF - DOWN_ROWS), :]

    def ag_wait(layer, mat):
        ag_got(layer, mat, 7, unit_rows(layer, mat, chip_at(7)))

    def run(calls):
        for fn, *where in calls:
            fn(*where)

    def hooked(b, hooks):
        for at, calls in hooks.items():
            @pl.when(b == at)
            def _(calls=calls):
                run(calls)

    def feature_rows(pos):
        return pl.ds(pl.multiple_of(chip_at(ARRIVAL[pos]) * FC, FC), FC)

    def forward_pass(layer, src, dst, lo, hi, hooks):
        final = layer == 1 and hi == NCHUNK

        def body(b, _):
            hooked(b, hooks)
            q, rows = token_rows(b)
            x = src[q, rows, :]
            hidden = dot_nn(x, jnp.concatenate([w1[layer, :, feature_rows(pos)] for pos in range(lo, hi)], axis=1))
            u, s = gelu_half(hidden)
            part = dot_nn((hidden * s).astype(BF16),
                          jnp.concatenate([w2[layer, feature_rows(pos), :] for pos in range(lo, hi)], axis=0))
            if lo > 0:
                part = part + dxa[q, rows, :]
            if hi < NCHUNK:
                dxa[q, rows, :] = part
            else:
                dst[q, rows, :] = (x.astype(F32) + part).astype(BF16)
            if final:
                @pl.when(q == 0)
                def _():
                    pltpu.make_async_copy(dst.at[0, rows, :], y_out.at[stage, 0, rows, :], y_sem.at[0]).start()

                @pl.when(q == 1)
                def _():
                    pltpu.make_async_remote_copy(src_ref=dst.at[1, rows, :], dst_ref=y_out.at[stage, 0, rows, :],
                                                 send_sem=y_sem.at[1], recv_sem=y_sem.at[2],
                                                 device_id=(partner,), device_id_type=MESH).start()
            return 0

        lax.fori_loop(0, 4, body, 0)

    r1, r2, r3 = round1, round2, round3

    rs_wait(1, 0)
    adam_up(1)
    round0(1, 0)
    rs_wait(1, 1)
    adam_dn(1)
    round0(1, 1)
    run(PRE(r1, r2, r3))
    rs_wait(0, 0)
    adam_up(0)
    round0(0, 0)
    rs_wait(0, 1)
    round1(0, 0)
    adam_dn(0)
    round0(0, 1)
    for layer in range(2):
        for mat in range(2):
            for c in out_copies(layer, mat):
                c.start()
    run(MID(r1, r2, r3))
    own_next.wait()
    pushes[3].wait_recv()
    for layer in range(2):
        for c in out_copies(layer, 1):
            c.wait()
    ag_wait(0, 0)
    run(BEFORE1A(r1, r2, r3))
    forward_pass(0, xs_top, xs_low, 0, 4, HOOKS1A(r1, r2, r3))
    ag_wait(0, 1)
    forward_pass(0, xs_top, xs_low, 4, 8, HOOKS1B(r1, r2, r3))
    run(BEFORE2A(r1, r2, r3))
    ag_wait(1, 0)
    forward_pass(1, xs_low, dyb, 0, 4, HOOKS2A(r1, r2, r3))
    ag_wait(1, 1)
    forward_pass(1, xs_low, dyb, 4, 8, {})

    for i in range(3):
        pltpu.make_async_copy(dyb.at[0], dyb.at[0], y_sem.at[i]).wait()
    for i in range(1, 4):
        pushes[i].wait_send()
    for layer in range(2):
        for mat in range(2):
            ref = rs_ref(layer, mat)
            pltpu.make_async_copy(ref, ref, rs_send.at[layer, mat]).wait()
            ref = ag_ref(layer, mat)
            pltpu.make_async_copy(ref, ref, ag_send.at[layer, mat]).wait()
            if mat == 0:
                for c in out_copies(layer, mat):
                    c.wait()


def emit_kernel(*refs):
    src, dst, buf = refs[:7], refs[7:14], refs[14:21]
    in_sem, done_sem = refs[21:]
    spots = [(i, half) for i in range(7) for half in range(2)]
    into = [pltpu.make_async_copy(src[i].at[h], buf[i].at[h], in_sem.at[i, h]) for i, h in spots]
    out = [pltpu.make_async_copy(buf[i].at[h], dst[i].at[h], done_sem.at[i, h]) for i, h in spots]
    for c in into:
        c.start()
    for c, d in zip(into, out):
        c.wait()
        d.start()
    for d in out:
        d.wait()


def solution(mesh):
    tok_spec = P(None, 'fsdp')
    layer_spec = P(None, None, 'fsdp')
    rep_spec = P()
    any_spec = pl.BlockSpec(memory_space=pl.ANY)
    up_state = (2, 2, UP_ROWS, FF)
    dn_state = (2, 2, DOWN_ROWS, D)
    sds = jax.ShapeDtypeStruct
    dma = pltpu.SemaphoreType.DMA

    call = pl.pallas_call(
        step_kernel,
        out_shape=(sds(up_state, F32), sds(dn_state, F32)) * 3 + (sds((2, 1, SEQ, D), BF16),),
        in_specs=[any_spec] * 13,
        out_specs=(any_spec,) * 7,
        scratch_shapes=[
            pltpu.VMEM((2, SEQ, D), BF16), pltpu.VMEM((2, SEQ, D), BF16), pltpu.VMEM((2, SEQ, D), BF16),
            pltpu.VMEM((2, SEQ, D), F32),
            pltpu.VMEM((2, D, FF), BF16), pltpu.VMEM((2, FF, D), BF16),
            pltpu.VMEM((2, NCHUNK, D, FC), BF16), pltpu.VMEM((2, FF, D), BF16),
            pltpu.VMEM((2, NCHUNK, D, FC), BF16), pltpu.VMEM((2, FF, D), BF16),
        ] + [pltpu.VMEM(up_state, F32)] * 4 + [
            pltpu.VMEM((2, 2, UP_ROWS, FF), BF16), pltpu.VMEM((2, 2, DOWN_ROWS, D), BF16),
            pltpu.VMEM((D, FC), F32), pltpu.VMEM((FC, D), F32),
            dma((27,)), dma((4,)), dma((4,)), dma((2, 2)), dma((2, 2)), dma((2, 2)), dma((2, 2, 8)),
            dma((2, 3, 3)), dma((3,)), pltpu.SemaphoreType.REGULAR,
        ],
        compiler_params=pltpu.CompilerParams(collective_id=0, has_side_effects=True, vmem_limit_bytes=67043328),
    )

    emit = pl.pallas_call(
        emit_kernel,
        out_shape=(sds(up_state, F32), sds(dn_state, F32)) * 3 + (sds((2, 1, SEQ, D), BF16),),
        in_specs=[any_spec] * 7,
        out_specs=(any_spec,) * 7,
        scratch_shapes=[pltpu.VMEM(up_state, F32), pltpu.VMEM(dn_state, F32)] * 3 + [pltpu.VMEM((2, 1, SEQ, D), BF16)] + [
            dma((7, 2)), dma((7, 2))],
        compiler_params=pltpu.CompilerParams(vmem_limit_bytes=67043328),
    )

    def device_step(*args):
        return emit(*call(*args))

    return jax.shard_map(device_step, mesh=mesh, in_specs=(layer_spec, tok_spec, tok_spec, rep_spec, rep_spec) + (layer_spec,) * 8,
                         out_specs=(layer_spec,) * 6 + (tok_spec,), check_vma=False)
```

```python
import jax
import jax.numpy as jnp
from jax import lax
from jax.experimental import pallas as pl
from jax.experimental.pallas import tpu as pltpu
from jax.sharding import PartitionSpec as P

LEARN_RATE = 0.005
BETA_ONE = 0.9
BETA_TWO = 0.95
ADAM_EPS = 1e-8
WEIGHT_DECAY = 0.1
MICROBATCHES = 2
ADAM_STEP = 2
CORR_ONE = 1.0 - BETA_ONE ** ADAM_STEP
CORR_TWO = 1.0 - BETA_TWO ** ADAM_STEP

GELU_A = 0.7978845608028654
GELU_B = 0.044715 * GELU_A

MESH = pl.DeviceIdType.MESH
BF16 = jnp.bfloat16
F32 = jnp.float32

NDEV = 16
SEQ = 2048
D = 512
FF = 2048
FC = 256
NCHUNK = FF // FC
UP_ROWS = D // NDEV
DOWN_ROWS = FF // NDEV
TB = 1024
SUB = 1024
ARRIVAL = (0, 1, 2, 4, 3, 6, 5, 7)
ORDER = (7, 6, 5, 3, 1, 2, 4, 0)


def PRE(r1, r2, r3):
    return [(r1, 1, 0)]


def MID(r1, r2, r3):
    return [(r2, 0, 0), (r1, 0, 1), (r3, 0, 0)]


def BEFORE1A(r1, r2, r3):
    return [(r2, 0, 1)]


def HOOKS1A(r1, r2, r3):
    return {1: [(r2, 1, 0)], 2: [(r3, 0, 1)]}


def HOOKS1B(r1, r2, r3):
    return {1: [(r1, 1, 1)], 2: [(r3, 1, 0)]}


def BEFORE2A(r1, r2, r3):
    return [(r2, 1, 1)]


def HOOKS2A(r1, r2, r3):
    return {3: [(r3, 1, 1)]}


def dot_nn(a, b):
    return lax.dot_general(a, b, (((1,), (0,)), ((), ())), preferred_element_type=F32)


def dot_nt(a, b):
    return lax.dot_general(a, b, (((1,), (1,)), ((), ())), preferred_element_type=F32)


def dot_tn(a, b):
    return lax.dot_general(a, b, (((0,), (0,)), ((), ())), preferred_element_type=F32)


def gelu_half(h):
    u = h * h
    return u, 0.5 * jnp.tanh(h * (GELU_B * u + GELU_A)) + 0.5


def gelu_and_grad(h, grad_act):
    u, s = gelu_half(h)
    g = h * s
    slope = s + (g - g * s) * ((6.0 * GELU_B) * u + 2.0 * GELU_A)
    return g.astype(BF16), (grad_act * slope).astype(BF16)


def adam_math(grad_sum, acc, master, mom, vel):
    grad_mean = (acc + grad_sum) / MICROBATCHES
    mom = BETA_ONE * mom + (1.0 - BETA_ONE) * grad_mean
    vel = BETA_TWO * vel + (1.0 - BETA_TWO) * grad_mean * grad_mean
    step_dir = (mom / CORR_ONE) / (jnp.sqrt(vel / CORR_TWO) + ADAM_EPS)
    master = master - LEARN_RATE * (step_dir + WEIGHT_DECAY * master)
    return master, mom, vel


def step_kernel(x_saved, grad_out, x_next, w_up, w_down, acc_up, acc_dn, mas_up, mas_dn, mo_up, mo_dn, ve_up, ve_dn,
                o_mas_up, o_mas_dn, o_mo_up, o_mo_dn, o_ve_up, o_ve_dn, y_out,
                xs_top, xs_low, dyb, dxa, w1, w2, sent_up, sent_dn, recv_up, recv_dn,
                s_acc_up, s_mas_up, s_mo_up, s_ve_up,
                own_up, own_dn, acc1, acc2,
                load_sem, tok_send, tok_recv, rs_send, rs_recv, ag_send, ag_recv, out_sem, y_sem, free_sem):
    me = lax.axis_index('fsdp')
    stage = lax.rem(me, 2)
    other = 1 - stage
    chip = me // 2
    partner = me + 1 - 2 * stage

    bits = (lax.rem(chip, 2), lax.rem(chip // 2, 2), chip // 4)

    def chip_xor(mask):
        flips = (lax.rem(mask, 2), lax.rem(mask // 2, 2), mask // 4)
        return sum(lax.rem(b + f, 2) * w for b, f, w in zip(bits, flips, (1, 2, 4)))

    def pick(table, i):
        return sum(jnp.where(i == k, v, 0) for k, v in enumerate(table))

    def chip_at(mask):
        return sum(((1 - b) if mask & w else b) * w for b, w in zip(bits, (1, 2, 4)))

    def load(i, src, dst):
        return pltpu.make_async_copy(src, dst, load_sem.at[i])

    loads = [
        load(0, w_up.at[stage, 1], w1.at[1]),
        load(1, x_saved.at[stage, 1, 0], xs_top.at[0]),
        load(2, w_down.at[stage, 1], w2.at[1]),
        load(3, grad_out.at[stage, 0], dyb.at[0]),
        load(4, w_up.at[stage, 0], w1.at[0]),
        load(5, x_saved.at[stage, 0, 0], xs_low.at[0]),
        load(6, w_down.at[stage, 0], w2.at[0]),
        load(7, acc_up, s_acc_up), load(8, mas_up, s_mas_up), load(9, mo_up, s_mo_up), load(10, ve_up, s_ve_up),
    ]

    def dn_rows(layer, arr, st):
        return ((layer * 4 + arr) * 2 + st) * DOWN_ROWS

    def dn_view(layer, arr, st):
        return dxa.at[0, pl.ds(dn_rows(layer, arr, st), DOWN_ROWS), :]

    dn_loads = [load(11 + arr * 4 + layer * 2 + st, src.at[st, layer], dn_view(layer, arr, st))
                for arr, src in enumerate((acc_dn, mas_dn, mo_dn, ve_dn)) for layer in range(2) for st in range(2)]
    for c in loads[:4]:
        c.start()

    barrier = pltpu.get_barrier_semaphore()

    def greet(t, _):
        pl.semaphore_signal(barrier, inc=1, device_id=(lax.rem(me + t, NDEV),), device_id_type=MESH)
        return 0

    lax.fori_loop(1, NDEV, greet, 0)
    pl.semaphore_wait(barrier, NDEV - 1)

    def push(i, src, dst):
        return pltpu.make_async_remote_copy(src_ref=src, dst_ref=dst, send_sem=tok_send.at[i], recv_sem=tok_recv.at[i],
                                            device_id=(partner,), device_id_type=MESH)

    pushes = [
        push(0, x_saved.at[other, 1, 0], xs_top.at[1]),
        push(1, grad_out.at[other, 0], dyb.at[1]),
        push(2, x_saved.at[other, 0, 0], xs_low.at[1]),
        push(3, x_next.at[other, 0], xs_top.at[1]),
    ]
    for c in pushes[:3]:
        c.start()
    for c in loads[4:]:
        c.start()

    for c in loads[:4]:
        c.wait()

    def down_rows(dev):
        return pl.ds(pl.multiple_of(dev * DOWN_ROWS, DOWN_ROWS), DOWN_ROWS)

    def send_up(layer, chunk, dest):
        return pltpu.make_async_remote_copy(
            src_ref=sent_up.at[layer, chunk, pl.ds(pl.multiple_of(dest * UP_ROWS, UP_ROWS), UP_ROWS), :],
            dst_ref=recv_up.at[layer, chunk, pl.ds(pl.multiple_of(me * UP_ROWS, UP_ROWS), UP_ROWS), :],
            send_sem=rs_send.at[layer, 0], recv_sem=rs_recv.at[layer, 0],
            device_id=(dest,), device_id_type=MESH)

    def send_dn(layer, chunk, core):
        dest = 2 * chunk + core
        return pltpu.make_async_remote_copy(
            src_ref=sent_dn.at[layer, down_rows(dest), :],
            dst_ref=recv_dn.at[layer, down_rows(me), :],
            send_sem=rs_send.at[layer, 1], recv_sem=rs_recv.at[layer, 1],
            device_id=(dest,), device_id_type=MESH)

    up_dests = [2 * chip_at(m) + core for m in ORDER[:-1] for core in range(2)] + [partner]

    def backward(layer, xs, with_dx, first_waits):
        def chunk_body(t, _, peeled=False):
            chunk = chip_xor(pick(ORDER, t))
            cols = pl.ds(pl.multiple_of(chunk * FC, FC), FC)

            def token_body(q):
                if q == 1 and peeled:
                    for c in first_waits:
                        c.wait_recv()

                x = xs[q]
                dy = dyb[q]
                tmp = sent_dn.at[0] if layer == 1 else xs_top.at[0]
                for lo in range(0, SEQ, SUB):
                    part_rows = slice(lo, lo + SUB)
                    hidden = dot_nn(x[part_rows], w1[layer, :, cols])
                    grad_act = dot_nt(dy[part_rows], w2[layer, cols, :])
                    tmp[part_rows, :FC], tmp[part_rows, FC:] = gelu_and_grad(hidden, grad_act)
                act = tmp[:, :FC]
                grad_hidden = tmp[:, FC:]
                part_dn = dot_tn(act, dy)
                part_up = dot_tn(x, grad_hidden)
                if q == 0:
                    acc2[...] = part_dn
                    acc1[...] = part_up
                else:
                    sent_dn[layer, cols, :] = (acc2[...] + part_dn).astype(BF16)
                    sent_up[layer, chunk] = (acc1[...] + part_up).astype(BF16)
                if with_dx:
                    part_x = dot_nt(grad_hidden, w1[layer, :, cols])
                    dxa[q] = part_x if peeled else dxa[q] + part_x

            token_body(0)
            token_body(1)

            @pl.when(t < NCHUNK - 1)
            def _():
                send_dn(layer, chunk, 0).start()
                send_dn(layer, chunk, 1).start()

            @pl.when(t == NCHUNK - 1)
            def _():
                send_dn(layer, chunk, other).start()
                recv_dn[layer, down_rows(me), :] = sent_dn[layer, down_rows(me), :]

            for dest in up_dests:
                send_up(layer, chunk, dest).start()
            own_rows = pl.ds(pl.multiple_of(me * UP_ROWS, UP_ROWS), UP_ROWS)
            recv_up[layer, chunk, own_rows, :] = sent_up[layer, chunk, own_rows, :]
            return 0

        if with_dx:
            chunk_body(0, 0, True)
        else:
            for c in first_waits:
                c.wait_recv()
        lax.fori_loop(1 if with_dx else 0, NCHUNK, chunk_body, 0)

    backward(1, xs_top, True, pushes[:2])
    pl.semaphore_signal(free_sem, inc=1, device_id=(partner,), device_id_type=MESH)

    def token_rows(b):
        return b // 2, pl.ds(pl.multiple_of(lax.rem(b, 2) * TB, TB), TB)

    def cot_body(b, _):
        q, rows = token_rows(b)
        dyb[q, rows, :] = (dyb[q, rows, :].astype(F32) + dxa[q, rows, :]).astype(BF16)
        return 0

    lax.fori_loop(0, 4, cot_body, 0)
    for c in dn_loads:
        c.start()
    for c in loads[4:7]:
        c.wait()
    backward(0, xs_low, False, pushes[2:3])

    own_next = load(1, x_next.at[stage, 0], xs_top.at[0])
    own_next.start()
    pl.semaphore_wait(free_sem, 1)
    pushes[0].wait_send()
    pushes[3].start()
    for c in loads[7:] + dn_loads:
        c.wait()

    def rs_ref(layer, mat):
        if mat == 0:
            return recv_up.at[layer, :, pl.ds(0, D - UP_ROWS), :]
        return recv_dn.at[layer, pl.ds(0, FF - DOWN_ROWS), :]

    def rs_wait(layer, mat):
        ref = rs_ref(layer, mat)
        pltpu.make_async_copy(ref, ref, rs_recv.at[layer, mat]).wait()

    def adam_up(layer):
        def body(chunk, _):
            cols = pl.ds(pl.multiple_of(chunk * FC, FC), FC)
            for st in range(2):
                total = recv_up[layer, chunk, pl.ds(st * UP_ROWS, UP_ROWS), :].astype(F32)
                for k in range(1, 8):
                    total = total + recv_up[layer, chunk, pl.ds((2 * k + st) * UP_ROWS, UP_ROWS), :].astype(F32)
                new = adam_math(total, s_acc_up[st, layer, :, cols], s_mas_up[st, layer, :, cols],
                                s_mo_up[st, layer, :, cols], s_ve_up[st, layer, :, cols])
                s_mas_up[st, layer, :, cols] = new[0]
                s_mo_up[st, layer, :, cols] = new[1]
                s_ve_up[st, layer, :, cols] = new[2]
                own_up[layer, st, :, cols] = new[0].astype(BF16)
            return 0

        lax.fori_loop(0, NCHUNK, body, 0)

    def adam_dn(layer):
        def body(r, _):
            rows = pl.ds(pl.multiple_of(r * 16, 16), 16)
            for st in range(2):
                from_dev = [pl.ds(pl.multiple_of((2 * k + st) * DOWN_ROWS + r * 16, 16), 16) for k in range(8)]
                total = recv_dn[layer, from_dev[0], :].astype(F32)
                for k in range(1, 8):
                    total = total + recv_dn[layer, from_dev[k], :].astype(F32)
                at = [pl.ds(pl.multiple_of(dn_rows(layer, arr, st) + r * 16, 16), 16) for arr in range(4)]
                new = adam_math(total, *(dxa[0, a, :] for a in at))
                for a, val in zip(at[1:], new):
                    dxa[0, a, :] = val
                own_dn[layer, st, rows, :] = new[0].astype(BF16)
            return 0

        lax.fori_loop(0, DOWN_ROWS // 16, body, 0)

    pairs_up = ((s_mas_up, o_mas_up), (s_mo_up, o_mo_up), (s_ve_up, o_ve_up))

    def out_copies(layer, mat):
        if mat == 0:
            return [pltpu.make_async_copy(src.at[:, layer], dst.at[:, layer], out_sem.at[layer, 0, i])
                    for i, (src, dst) in enumerate(pairs_up)]
        return [pltpu.make_async_copy(dn_view(layer, i + 1, st), dst.at[st, layer], out_sem.at[layer, 1 + st, i])
                for i, dst in enumerate((o_mas_dn, o_mo_dn, o_ve_dn)) for st in range(2)]

    def piece_rows(layer, mat, dev):
        if mat == 0:
            return w1.at[layer, pl.ds(pl.multiple_of(dev * UP_ROWS, UP_ROWS), UP_ROWS), :]
        return w2.at[layer, pl.ds(pl.multiple_of(dev * DOWN_ROWS, DOWN_ROWS), DOWN_ROWS), :]

    def unit_rows(layer, mat, owner, part=None):
        full, size, cuts = ((w1, 2 * UP_ROWS, (0, 32, 48, 64)), (w2, 2 * DOWN_ROWS, (0, 96, 176, 256)))[mat]
        lo, hi = (0, size) if part is None else cuts[part:part + 2]
        return full.at[layer, pl.ds(pl.multiple_of(owner * size + lo, 16), hi - lo), :]

    def ag_copy(layer, mat, src, dst, slot, dest):
        return pltpu.make_async_remote_copy(src_ref=src, dst_ref=dst, send_sem=ag_send.at[layer, mat],
                                            recv_sem=ag_recv.at[layer, mat, slot],
                                            device_id=(dest,), device_id_type=MESH)

    def ag_got(layer, mat, slot, ref):
        pltpu.make_async_copy(ref, ref, ag_recv.at[layer, mat, slot]).wait()

    def round0(layer, mat):
        own = (own_up, own_dn)[mat]
        ag_copy(layer, mat, own.at[layer, other], piece_rows(layer, mat, me), 0, partner).start()
        piece_rows(layer, mat, me)[...] = own[layer, stage]

    def neighbour(mask):
        return 2 * chip_at(mask) + stage

    def send_unit(layer, mat, owner, slot, mask, part=None):
        ref = unit_rows(layer, mat, chip_at(owner), part)
        ag_copy(layer, mat, ref, ref, slot, neighbour(mask)).start()

    def round1(layer, mat):
        ag_got(layer, mat, 0, piece_rows(layer, mat, partner))
        for i in range(3):
            send_unit(layer, mat, 0, 1 + i, 1 << i)

    def round2(layer, mat):
        for link, came in ((0, 1), (1, 2), (2, 0)):
            ag_got(layer, mat, 1 + came, unit_rows(layer, mat, chip_at(1 << came)))
            send_unit(layer, mat, 1 << came, 4 + link, 1 << link)

    def round3(layer, mat):
        for link, owner, came in ((2, 3, 0), (0, 6, 1), (1, 5, 2)):
            ag_got(layer, mat, 4 + came, unit_rows(layer, mat, chip_at(owner)))
            send_unit(layer, mat, owner, 7, 1 << link, link)

    def ag_ref(layer, mat):
        if mat == 0:
            return w1.at[layer, pl.ds(0, D - UP_ROWS), :]
        return w2.at[layer, pl.ds(0, FF - DOWN_ROWS), :]

    def ag_wait(layer, mat):
        ag_got(layer, mat, 7, unit_rows(layer, mat, chip_at(7)))

    def run(calls):
        for fn, *where in calls:
            fn(*where)

    def hooked(b, hooks):
        for at, calls in hooks.items():
            @pl.when(b == at)
            def _(calls=calls):
                run(calls)

    def feature_rows(pos):
        return pl.ds(pl.multiple_of(chip_at(ARRIVAL[pos]) * FC, FC), FC)

    def forward_pass(layer, src, dst, lo, hi, hooks):
        final = layer == 1 and hi == NCHUNK

        def body(b, _):
            hooked(b, hooks)
            q, rows = token_rows(b)
            x = src[q, rows, :]
            hidden = dot_nn(x, jnp.concatenate([w1[layer, :, feature_rows(pos)] for pos in range(lo, hi)], axis=1))
            u, s = gelu_half(hidden)
            part = dot_nn((hidden * s).astype(BF16),
                          jnp.concatenate([w2[layer, feature_rows(pos), :] for pos in range(lo, hi)], axis=0))
            if lo > 0:
                part = part + dxa[q, rows, :]
            if hi < NCHUNK:
                dxa[q, rows, :] = part
            else:
                dst[q, rows, :] = (x.astype(F32) + part).astype(BF16)
            if final:
                @pl.when(q == 0)
                def _():
                    pltpu.make_async_copy(dst.at[0, rows, :], y_out.at[stage, 0, rows, :], y_sem.at[0]).start()

                @pl.when(q == 1)
                def _():
                    pltpu.make_async_remote_copy(src_ref=dst.at[1, rows, :], dst_ref=y_out.at[stage, 0, rows, :],
                                                 send_sem=y_sem.at[1], recv_sem=y_sem.at[2],
                                                 device_id=(partner,), device_id_type=MESH).start()
            return 0

        lax.fori_loop(0, 4, body, 0)

    r1, r2, r3 = round1, round2, round3

    rs_wait(1, 0)
    adam_up(1)
    round0(1, 0)
    rs_wait(1, 1)
    adam_dn(1)
    round0(1, 1)
    run(PRE(r1, r2, r3))
    rs_wait(0, 0)
    adam_up(0)
    round0(0, 0)
    rs_wait(0, 1)
    round1(0, 0)
    adam_dn(0)
    round0(0, 1)
    for layer in range(2):
        for mat in range(2):
            for c in out_copies(layer, mat):
                c.start()
    run(MID(r1, r2, r3))
    own_next.wait()
    pushes[3].wait_recv()
    for layer in range(2):
        for c in out_copies(layer, 1):
            c.wait()
    ag_wait(0, 0)
    run(BEFORE1A(r1, r2, r3))
    forward_pass(0, xs_top, xs_low, 0, 4, HOOKS1A(r1, r2, r3))
    ag_wait(0, 1)
    forward_pass(0, xs_top, xs_low, 4, 8, HOOKS1B(r1, r2, r3))
    run(BEFORE2A(r1, r2, r3))
    ag_wait(1, 0)
    forward_pass(1, xs_low, dyb, 0, 4, HOOKS2A(r1, r2, r3))
    ag_wait(1, 1)
    forward_pass(1, xs_low, dyb, 4, 8, {})

    for i in range(3):
        pltpu.make_async_copy(dyb.at[0], dyb.at[0], y_sem.at[i]).wait()
    for i in range(1, 4):
        pushes[i].wait_send()
    for layer in range(2):
        for mat in range(2):
            ref = rs_ref(layer, mat)
            pltpu.make_async_copy(ref, ref, rs_send.at[layer, mat]).wait()
            ref = ag_ref(layer, mat)
            pltpu.make_async_copy(ref, ref, ag_send.at[layer, mat]).wait()
            if mat == 0:
                for c in out_copies(layer, mat):
                    c.wait()


def emit_kernel(*refs):
    src, dst, buf = refs[:7], refs[7:14], refs[14:21]
    in_sem, done_sem = refs[21:]
    spots = [(i, h, j) for i in range(7) for h in range(2) for j in range(2)]

    def piece(ref, i, h, j):
        return ref.at[h, j] if i < 6 else ref.at[h, 0, pl.ds(j * (SEQ // 2), SEQ // 2), :]

    into = [pltpu.make_async_copy(piece(src[i], i, h, j), piece(buf[i], i, h, j), in_sem.at[i, h, j]) for i, h, j in spots]
    out = [pltpu.make_async_copy(piece(buf[i], i, h, j), piece(dst[i], i, h, j), done_sem.at[i, h, j]) for i, h, j in spots]
    for c in into:
        c.start()
    for c, d in zip(into, out):
        c.wait()
        d.start()
    for d in out:
        d.wait()


def solution(mesh):
    tok_spec = P(None, 'fsdp')
    layer_spec = P(None, None, 'fsdp')
    rep_spec = P()
    any_spec = pl.BlockSpec(memory_space=pl.ANY)
    up_state = (2, 2, UP_ROWS, FF)
    dn_state = (2, 2, DOWN_ROWS, D)
    sds = jax.ShapeDtypeStruct
    dma = pltpu.SemaphoreType.DMA

    call = pl.pallas_call(
        step_kernel,
        out_shape=(sds(up_state, F32), sds(dn_state, F32)) * 3 + (sds((2, 1, SEQ, D), BF16),),
        in_specs=[any_spec] * 13,
        out_specs=(any_spec,) * 7,
        scratch_shapes=[
            pltpu.VMEM((2, SEQ, D), BF16), pltpu.VMEM((2, SEQ, D), BF16), pltpu.VMEM((2, SEQ, D), BF16),
            pltpu.VMEM((2, SEQ, D), F32),
            pltpu.VMEM((2, D, FF), BF16), pltpu.VMEM((2, FF, D), BF16),
            pltpu.VMEM((2, NCHUNK, D, FC), BF16), pltpu.VMEM((2, FF, D), BF16),
            pltpu.VMEM((2, NCHUNK, D, FC), BF16), pltpu.VMEM((2, FF, D), BF16),
        ] + [pltpu.VMEM(up_state, F32)] * 4 + [
            pltpu.VMEM((2, 2, UP_ROWS, FF), BF16), pltpu.VMEM((2, 2, DOWN_ROWS, D), BF16),
            pltpu.VMEM((D, FC), F32), pltpu.VMEM((FC, D), F32),
            dma((27,)), dma((4,)), dma((4,)), dma((2, 2)), dma((2, 2)), dma((2, 2)), dma((2, 2, 8)),
            dma((2, 3, 3)), dma((3,)), pltpu.SemaphoreType.REGULAR,
        ],
        compiler_params=pltpu.CompilerParams(collective_id=0, has_side_effects=True, vmem_limit_bytes=67043328),
    )

    emit = pl.pallas_call(
        emit_kernel,
        out_shape=(sds(up_state, F32), sds(dn_state, F32)) * 3 + (sds((2, 1, SEQ, D), BF16),),
        in_specs=[any_spec] * 7,
        out_specs=(any_spec,) * 7,
        scratch_shapes=[pltpu.VMEM(up_state, F32), pltpu.VMEM(dn_state, F32)] * 3 + [pltpu.VMEM((2, 1, SEQ, D), BF16)] + [
            dma((7, 2, 2)), dma((7, 2, 2))],
        compiler_params=pltpu.CompilerParams(vmem_limit_bytes=67043328),
    )

    def device_step(*args):
        return emit(*call(*args))

    return jax.shard_map(device_step, mesh=mesh, in_specs=(layer_spec, tok_spec, tok_spec, rep_spec, rep_spec) + (layer_spec,) * 8,
                         out_specs=(layer_spec,) * 6 + (tok_spec,), check_vma=False)
```
